512 devices in a mesh: head: 16 (over y, core), seq: 32 (over x, z).
Axes of the slice: x: 4, y: 8, z: 8, core: 2. Of those that a mesh axis runs over, the one named last changes fastest.
Arguments:
- layer_input: bfloat16 [4096, 4096], P('seq', 'head'), may hold values from -6 to 6
- receptance: bfloat16 [4096, 4096], P('seq', 'head'), may hold values from -6 to 6
- key_act: bfloat16 [4096, 4096], P('seq', 'head'), may hold values from -0.75 to 0.75
- value_act: bfloat16 [4096, 4096], P('seq', 'head'), may hold values from -6 to 6
- attention_result_sensitivity: bfloat16 [4096, 4096], P('seq', 'head'), may hold values from -0.625 to 0.625
- time_first: float32 [64, 64], P('head'), may hold values from -1 to 1
- decay_exponent_base: float32 [4096], P('head'), may hold values from -9 to -3.4
- decay_shift_mix: float32 [4096], P('head'), may hold values from 0 to 1
- mix_rkv: float32 [3, 4096], replicated, may hold values from 0 to 1
- decay_adapter_down: float32 [4096, 128], P('head'), may hold values from -0.09375 to 0.09375
- decay_adapter_up: float32 [128, 4096], P(None, 'head'), may hold values from -1 to 1
- proj_weights: bfloat16 [3, 4096, 4096], P(None, 'seq', 'head'), may hold values from -0.09375 to 0.09375
Outputs:
- stratum_source_sensitivity: bfloat16 [4096, 4096], P('seq', 'head')
- decay_down_grad: float32 [4096, 128], P('head')
- decay_up_grad: float32 [128, 4096], P(None, 'head')
- decay_base_grad: float32 [4096], P('head')
- time_first_grad: float32 [64, 64], P('head')
The draws below stay inside these ranges and needn't reach their ends.
All inputs are finite; a program needn't handle non-finite values.
Results may differ from the reference program's by a relative error of at most 0.018.
Values may be sent and summed in bfloat16 or wider, within the bound.
A program may use at most 64 MiB of HBM per device.

```python
import jax
import jax.numpy as jnp
from jax import lax

MODEL_WIDTH = 4096
HEADS = 64
HS = 64
ADAPTER_RANK = 128
TOK_DEV = 128
TOKENS = 4096
N_HEAD = 16


def steps_of(key, extent, split, smallest, largest):
    def one(dim, blocks):
        heights = jax.random.uniform(jax.random.fold_in(jax.random.fold_in(key, 6), dim), (blocks,), jnp.float32, smallest / len(split), largest / len(split))
        return jnp.repeat(jnp.exp(heights), extent[dim] // blocks).reshape((-1,) + (1,) * (len(extent) - dim - 1))

    factor_of = one(*split[0])
    for cut in split[1:]:
        factor_of = factor_of * one(*cut)
    return factor_of


def gaussian(stream_key, extent, deviation, reach, cuts=(), held_as=jnp.bfloat16):
    gain = steps_of(stream_key, extent, cuts, -0.22, 0.18) if cuts else 1.0
    entries = jax.random.normal(stream_key, extent, jnp.float32) * deviation * gain
    return jnp.minimum(jnp.maximum(entries, -reach), reach).astype(held_as)


def setup_inputs(seed: int = 0) -> dict:
    key_of = jax.random.split(jax.random.key(seed), 13)
    return {
        "layer_input": gaussian(key_of[0], (TOKENS, MODEL_WIDTH), 1.0, 6.0, ((0, 32), (1, 16))),
        "receptance": gaussian(key_of[1], (TOKENS, MODEL_WIDTH), 1.0, 6.0, ((0, 32), (1, 16))),
        "key_act": gaussian(key_of[2], (TOKENS, MODEL_WIDTH), 0.125, 0.75, ((0, 32), (1, 16))),
        "value_act": gaussian(key_of[3], (TOKENS, MODEL_WIDTH), 1.0, 6.0, ((0, 32), (1, 16))),
        "attention_result_sensitivity": gaussian(key_of[4], (TOKENS, MODEL_WIDTH), 0.1, 0.625, ((0, 32), (1, 16))),
        "time_first": jnp.clip(jax.random.uniform(key_of[5], (HEADS, HS), jnp.float32, -1.0, 1.0) * steps_of(key_of[5], (HEADS, HS), ((0, 16),), -0.4, 0.0), -1.0, 1.0),
        "decay_exponent_base": jnp.clip(-9.0 + 5.6 * jax.random.uniform(key_of[6], (MODEL_WIDTH,), jnp.float32) ** steps_of(key_of[6], (MODEL_WIDTH,), ((0, 16),), -0.2, 0.2), -9.0, -3.4),
        "decay_shift_mix": jnp.clip(1.0 * jax.random.uniform(key_of[7], (MODEL_WIDTH,), jnp.float32) ** steps_of(key_of[7], (MODEL_WIDTH,), ((0, 16),), -0.2, 0.2), 0.0, 1.0),
        "mix_rkv": jnp.clip(jax.random.uniform(key_of[8], (3, MODEL_WIDTH), jnp.float32, 0.0, 1.0), 0.0, 1.0),
        "decay_adapter_down": gaussian(key_of[9], (MODEL_WIDTH, ADAPTER_RANK), MODEL_WIDTH ** -0.5, 0.09375, ((0, 16),), jnp.float32),
        "decay_adapter_up": gaussian(key_of[10], (ADAPTER_RANK, MODEL_WIDTH), 0.18, 1.0, ((1, 16),), jnp.float32),
        "proj_weights": gaussian(key_of[11], (3, MODEL_WIDTH, MODEL_WIDTH), MODEL_WIDTH ** -0.5, 0.09375, ((1, 32), (2, 16))),
    }


EXACT_ARITHMETIC = lax.Precision.HIGHEST

def onward_scan_loop(gate_matrix, lookup_matrix, payload_matrix, fading_natural_scale, initial_reward):

    def advance(memory_matrix_handed, sequence_entries):
        present_gate_vector, key_now, val_now, logd_now = sequence_entries
        lookup_payload_product = key_now[:, :, None] * val_now[:, None, :]
        attention_result = jnp.einsum('uk,ukv->uv', present_gate_vector, memory_matrix_handed + initial_reward[:, :, None] * lookup_payload_product, precision=EXACT_ARITHMETIC)
        memory_matrix_handed = jnp.exp(logd_now)[:, :, None] * memory_matrix_handed + lookup_payload_product
        return (memory_matrix_handed, attention_result)

    def segment(memory_matrix_handed, sequence_entries):
        return lax.scan(advance, memory_matrix_handed, sequence_entries)
    length_all, head_count, head_size = gate_matrix.shape
    pieces = length_all // TOK_DEV

    def to_blocks(array):
        return array.reshape(pieces, TOK_DEV, head_count, head_size)
    initial = jnp.zeros((head_count, head_size, head_size), gate_matrix.dtype)
    unused, outputs = lax.scan(jax.checkpoint(segment), initial, (to_blocks(gate_matrix), to_blocks(lookup_matrix), to_blocks(payload_matrix), to_blocks(fading_natural_scale)))
    return outputs.reshape(length_all, head_count, head_size)

def reference(layer_input, receptance, key_act, value_act, attention_result_sensitivity, time_first, decay_exponent_base, decay_shift_mix, mix_rkv, decay_adapter_down, decay_adapter_up, proj_weights):
    features = layer_input.astype(jnp.float32)
    length_all = features.shape[0]
    previous = jnp.concatenate([jnp.zeros((1, MODEL_WIDTH), jnp.float32), features[:-1]], 0)
    decay_input = features + decay_shift_mix * (previous - features)
    adapter_middle = jnp.tanh(jnp.dot(decay_input, decay_adapter_down, precision=EXACT_ARITHMETIC))
    fading_natural_scale = -jnp.exp(decay_exponent_base + jnp.dot(adapter_middle, decay_adapter_up, precision=EXACT_ARITHMETIC))

    def attention_partition(array):
        return array.astype(jnp.float32).reshape(length_all, HEADS, HS)
    unused_out, reverse_mode_map = jax.vjp(onward_scan_loop, attention_partition(receptance), attention_partition(key_act), attention_partition(value_act), fading_natural_scale.reshape(length_all, HEADS, HS), time_first)
    gate_sensitivity, lookup_sensitivity, payload_sensitivity, fading_scale_sensitivity, reward_sensitivity = reverse_mode_map(attention_partition(attention_result_sensitivity))
    preactivation_gradient = fading_scale_sensitivity.reshape(length_all, MODEL_WIDTH) * fading_natural_scale
    raising_matrix_sensitivity = jnp.dot(adapter_middle.T, preactivation_gradient, precision=EXACT_ARITHMETIC)
    floor_rate_sensitivity = lax.optimization_barrier(jnp.sum(preactivation_gradient, 0))
    middle_gradient = jnp.dot(preactivation_gradient, decay_adapter_up.T, precision=EXACT_ARITHMETIC) * (1.0 - adapter_middle * adapter_middle)
    lowering_matrix_sensitivity = jnp.dot(decay_input.T, middle_gradient, precision=EXACT_ARITHMETIC)
    decay_input_gradient = jnp.dot(middle_gradient, decay_adapter_down.T, precision=EXACT_ARITHMETIC)
    projected = jnp.stack([gate_sensitivity.reshape(length_all, MODEL_WIDTH), lookup_sensitivity.reshape(length_all, MODEL_WIDTH), payload_sensitivity.reshape(length_all, MODEL_WIDTH)]).astype(jnp.bfloat16)
    group_columns = MODEL_WIDTH // N_HEAD

    def add_group(index, accum):
        token_offset = (index * group_columns).astype(jnp.int32)
        own_portion = jnp.zeros((length_all, MODEL_WIDTH), jnp.float32)
        previous_portion = jnp.zeros((length_all, MODEL_WIDTH), jnp.float32)
        for member in range(3):
            piece_grad = lax.dynamic_slice_in_dim(projected[member], token_offset, group_columns, 1).astype(jnp.float32)
            piece_weight = lax.dynamic_slice_in_dim(proj_weights[member], token_offset, group_columns, 1).astype(jnp.float32)
            term = jnp.dot(piece_grad, piece_weight.T, precision=EXACT_ARITHMETIC)
            own_portion = own_portion + (1.0 - mix_rkv[member]) * term
            previous_portion = previous_portion + mix_rkv[member] * term
        adapter_columns = lax.dynamic_slice_in_dim(decay_input_gradient, token_offset, group_columns, 1)
        mixed_columns = lax.dynamic_slice_in_dim(decay_shift_mix, token_offset, group_columns, 0)
        own_columns = lax.dynamic_slice_in_dim(own_portion, token_offset, group_columns, 1) + (1.0 - mixed_columns) * adapter_columns
        own_portion = lax.dynamic_update_slice_in_dim(own_portion, own_columns, token_offset, 1)
        previous_columns = lax.dynamic_slice_in_dim(previous_portion, token_offset, group_columns, 1) + mixed_columns * adapter_columns
        previous_portion = lax.dynamic_update_slice_in_dim(previous_portion, previous_columns, token_offset, 1)
        group_term = own_portion + jnp.concatenate([previous_portion[1:], jnp.zeros((1, MODEL_WIDTH), jnp.float32)], 0)
        rounded = lax.optimization_barrier(group_term.astype(jnp.bfloat16))
        return accum + rounded.astype(jnp.float32)
    accumulated_contributions = lax.fori_loop(0, N_HEAD, add_group, jnp.zeros((length_all, MODEL_WIDTH), jnp.float32))
    return (accumulated_contributions.astype(jnp.bfloat16), lowering_matrix_sensitivity, raising_matrix_sensitivity, floor_rate_sensitivity, reward_sensitivity)
```

```python
from functools import partial

import jax
import jax.numpy as jnp
from jax import lax
from jax.experimental import pallas as pl
from jax.experimental.pallas import tpu as pltpu
from jax.sharding import PartitionSpec as P

F32 = jnp.float32
BF16 = jnp.bfloat16
MESH = pl.DeviceIdType.MESH
N_HEAD = 16
N_SEQ = 32
TOK = 128
COL = 256
HS = 64
RANK = 128
VMEM = pl.BlockSpec(memory_space=pltpu.VMEM)

ROWS_LANES = (((1,), (0,)), ((), ()))
LANES_LANES = (((1,), (1,)), ((), ()))


def mm(a, b, dims=ROWS_LANES):
    return lax.dot_general(a, b, dims, preferred_element_type=F32)


def parts(a, count):
    out = []
    for _ in range(count - 1):
        top = a.astype(BF16)
        out.append(top)
        a = a - top.astype(F32)
    out.append(a.astype(BF16))
    return out


def mm3(a, b, dims=ROWS_LANES):
    ah, al = parts(a, 2)
    bh, bl = parts(b, 2)
    return mm(ah, bh, dims) + (mm(ah, bl, dims) + mm(al, bh, dims))


def mm_right_exact(a, b, dims=ROWS_LANES, count=2):
    out = None
    for piece in parts(a, count):
        term = mm(piece, b, dims)
        out = term if out is None else out + term
    return out


def mm_left_exact(a, b, dims=ROWS_LANES, count=2):
    out = None
    for piece in parts(b, count):
        term = mm(a, piece, dims)
        out = term if out is None else out + term
    return out


def iota(shape, dim):
    return lax.broadcasted_iota(jnp.int32, shape, dim)


def head_of(index):
    return index // HS


def lower_ones(strict):
    row, col = iota((TOK, TOK), 0), iota((TOK, TOK), 1)
    keep = row > col if strict else row >= col
    return jnp.where(keep, 1.0, 0.0).astype(BF16)


def upper_ones():
    row, col = iota((TOK, TOK), 0), iota((TOK, TOK), 1)
    return jnp.where(row < col, 1.0, 0.0).astype(BF16)


def block_diagonal():
    return head_of(iota((COL, COL), 0)) == head_of(iota((COL, COL), 1))


def odd_rows():
    return (head_of(iota((COL, 128), 0)) % 2) == 1


def remote(src, dst, send_sem, recv_sem, to):
    return pltpu.make_async_remote_copy(
        src_ref=src, dst_ref=dst, send_sem=send_sem, recv_sem=recv_sem,
        device_id=to, device_id_type=MESH,
    )


def greet(barrier, to):
    pl.semaphore_signal(barrier, inc=1, device_id=to, device_id_type=MESH)


def comm_params(ident):
    return pltpu.CompilerParams(collective_id=ident, has_side_effects=True)


def loop(start, stop, body):
    def step(i, carry):
        body(i)
        return carry

    lax.fori_loop(start, stop, step, 0)


def head_total(me, part, land, full, sems):
    send1, recv1, send2, recv2 = sems

    def first(d):
        to = (me + d) % N_HEAD
        return remote(part.at[to], land.at[me], send1.at[to], recv1.at[me], {"head": to})

    def first_in(d):
        frm = (me + d) % N_HEAD
        return remote(part.at[frm], land.at[frm], send1.at[frm], recv1.at[frm], {"head": frm})

    def second(d):
        to = (me + d) % N_HEAD
        return remote(full.at[me], full.at[me], send2.at[to], recv2.at[me], {"head": to})

    def second_in(d):
        frm = (me + d) % N_HEAD
        return remote(full.at[frm], full.at[frm], send2.at[frm], recv2.at[frm], {"head": frm})

    loop(1, N_HEAD, lambda d: first(d).start())
    land[me] = part[me]
    loop(1, N_HEAD, lambda d: first_in(d).wait_recv())
    total = land[0]
    for j in range(1, N_HEAD):
        total = total + land[j]
    full[me] = total
    loop(1, N_HEAD, lambda d: second(d).start())

    def finish():
        loop(1, N_HEAD, lambda d: second_in(d).wait_recv())
        loop(1, N_HEAD, lambda d: first_in(d).wait_send())
        loop(1, N_HEAD, lambda d: second_in(d).wait_send())

    return finish


HEAD_SCRATCH = [
    pltpu.VMEM((N_HEAD, 8, 128), F32),
    pltpu.VMEM((N_HEAD, 8, 128), F32),
    pltpu.VMEM((N_HEAD, 8, 128), F32),
    pltpu.SemaphoreType.DMA((N_HEAD,)),
    pltpu.SemaphoreType.DMA((N_HEAD,)),
    pltpu.SemaphoreType.DMA((N_HEAD,)),
    pltpu.SemaphoreType.DMA((N_HEAD,)),
]


def shift_mix(x, carried, mix):
    previous = pltpu.roll(x, 1, 0)
    previous = jnp.where(iota((TOK, COL), 0) == 0, carried, previous)
    return x + mix * (previous - x)


def adapter_in_kernel(
    x_ref, mix_ref, down_ref, pre_ref, row_ref,
    tail, part, land, full, send1, recv1, send2, recv2, row_send, row_recv,
):
    h, s = lax.axis_index("head"), lax.axis_index("seq")
    after, ahead = (s + 1) % N_SEQ, (s + N_SEQ - 1) % N_SEQ
    barrier = pltpu.get_barrier_semaphore()
    loop(1, N_HEAD, lambda d: greet(barrier, {"head": (h + d) % N_HEAD}))
    greet(barrier, {"seq": after})
    greet(barrier, {"seq": ahead})
    pl.semaphore_wait(barrier, N_HEAD + 1)
    copy = remote(x_ref.at[pl.ds(TOK - 16, 16)], tail, row_send, row_recv, {"seq": after})
    copy.start()
    x = x_ref[...].astype(F32)
    mix = mix_ref[...]
    copy.wait()
    carried = jnp.where(s == 0, 0.0, tail[...].astype(F32)[15:16])
    row_ref[...] = jnp.broadcast_to(carried, (8, COL))
    value = mm3(shift_mix(x, carried, mix), down_ref[...])
    part[...] = value.reshape(N_HEAD, 8, 128)
    head_total(h, part, land, full, (send1, recv1, send2, recv2))()
    pre_ref[...] = full[...].reshape(TOK, RANK)


def adapter_in(x, mix, down):
    return pl.pallas_call(
        adapter_in_kernel,
        out_shape=(
            jax.ShapeDtypeStruct((TOK, RANK), F32),
            jax.ShapeDtypeStruct((8, COL), F32),
        ),
        in_specs=[VMEM] * 3,
        out_specs=(VMEM, VMEM),
        scratch_shapes=[pltpu.VMEM((16, COL), BF16), *HEAD_SCRATCH,
                        pltpu.SemaphoreType.DMA, pltpu.SemaphoreType.DMA],
        compiler_params=comm_params(0),
        cost_estimate=pl.CostEstimate(flops=10**10, bytes_accessed=10**5, transcendentals=0),
        name="adapter_in",
    )(x, mix, down)


def local_kernel(pre_ref, base_ref, up_ref, r_ref, k_ref, v_ref, dy_ref, mid_ref, w_ref, cum_ref, pack_ref):
    mid = jnp.tanh(pre_ref[...])
    mid_ref[...] = mid
    w = -jnp.exp(base_ref[...] + mm3(mid, up_ref[...]))
    w_ref[...] = w
    w_parts = parts(w, 3)
    ones = lower_ones(False)
    cumul = mm(ones, w_parts[0]) + (mm(ones, w_parts[1]) + mm(ones, w_parts[2]))
    cum_ref[...] = cumul
    before = cumul - w
    final = cumul[TOK - 1 : TOK]
    flat = jnp.ones((TOK, 128), BF16)
    w_t = [p.astype(F32).T.astype(BF16) for p in w_parts]
    total_rows = mm(w_t[0], flat) + (mm(w_t[1], flat) + mm(w_t[2], flat))
    to_end = jnp.exp(jnp.minimum(final - cumul, 0.0))
    own = block_diagonal()
    odd = odd_rows()

    def folded(left, right):
        wide = mm_right_exact(left.T, right)
        wide = jnp.where(own, wide, 0.0)
        return wide[:, :128] + wide[:, 128:]

    state = folded(k_ref[...].astype(F32) * to_end, v_ref[...])
    grad = folded(r_ref[...].astype(F32) * jnp.exp(before), dy_ref[...])
    packed = jnp.where(odd, pltpu.roll(state, 64, 1), state) + jnp.where(odd, grad, pltpu.roll(grad, 64, 1))
    pack_ref[:, 0] = packed.reshape(N_SEQ, 8, 128)
    pack_ref[:, 1] = jnp.exp(total_rows).reshape(N_SEQ, 8, 128)


def local_terms(pre, base, up, r, k, v, dy):
    wide = jax.ShapeDtypeStruct((TOK, COL), F32)
    return pl.pallas_call(
        local_kernel,
        out_shape=(jax.ShapeDtypeStruct((TOK, RANK), F32), wide, wide,
                   jax.ShapeDtypeStruct((N_SEQ, 2, 8, 128), F32)),
        in_specs=[VMEM] * 7,
        out_specs=(VMEM,) * 4,
        cost_estimate=pl.CostEstimate(flops=10**10, bytes_accessed=10**6, transcendentals=0),
        name="local_terms",
    )(pre, base, up, r, k, v, dy)


def state_kernel(pack_ref, out_ref, land, back, got, send1, recv1, send2, recv2):
    s = lax.axis_index("seq")
    barrier = pltpu.get_barrier_semaphore()
    loop(1, N_SEQ, lambda d: greet(barrier, {"seq": (s + d) % N_SEQ}))
    pl.semaphore_wait(barrier, N_SEQ - 1)

    def first(d):
        to = (s + d) % N_SEQ
        return remote(pack_ref.at[to], land.at[s], send1.at[to], recv1.at[s], {"seq": to})

    def first_in(d):
        frm = (s + d) % N_SEQ
        return remote(pack_ref.at[frm], land.at[frm], send1.at[frm], recv1.at[frm], {"seq": frm})

    def second(d):
        to = (s + d) % N_SEQ
        return remote(back.at[to], got.at[s], send2.at[to], recv2.at[s], {"seq": to})

    def second_in(d):
        frm = (s + d) % N_SEQ
        return remote(back.at[frm], got.at[frm], send2.at[frm], recv2.at[frm], {"seq": frm})

    loop(1, N_SEQ, lambda d: first(d).start())
    land[s] = pack_ref[s]
    loop(1, N_SEQ, lambda d: first_in(d).wait_recv())
    onward = jnp.zeros((8, 128), F32)
    forward = []
    for n in range(N_SEQ):
        forward.append(onward)
        onward = land[n, 1] * onward + land[n, 0]
    left = iota((8, 128), 1) < 64
    reverse = jnp.zeros((8, 128), F32)
    for n in reversed(range(N_SEQ)):
        back[n] = jnp.where(left, forward[n], reverse)
        reverse = land[n, 1] * reverse + land[n, 0]
    loop(1, N_SEQ, lambda d: second(d).start())
    got[s] = back[s]
    loop(1, N_SEQ, lambda d: second_in(d).wait_recv())
    out_ref[...] = got[...].reshape(COL, 128)
    loop(1, N_SEQ, lambda d: first_in(d).wait_send())
    loop(1, N_SEQ, lambda d: second_in(d).wait_send())


def state_exchange(pack):
    return pl.pallas_call(
        state_kernel,
        out_shape=jax.ShapeDtypeStruct((COL, 128), F32),
        in_specs=[VMEM],
        out_specs=VMEM,
        scratch_shapes=[
            pltpu.VMEM((N_SEQ, 2, 8, 128), F32),
            pltpu.VMEM((N_SEQ, 8, 128), F32),
            pltpu.VMEM((N_SEQ, 8, 128), F32),
            *[pltpu.SemaphoreType.DMA((N_SEQ,))] * 4,
        ],
        compiler_params=comm_params(1),
        cost_estimate=pl.CostEstimate(flops=10**10, bytes_accessed=10**5, transcendentals=0),
        name="state_exchange",
    )(pack)


def lane_cat(stacked):
    return jnp.concatenate([stacked[h * TOK : (h + 1) * TOK] for h in range(4)], axis=1)


def wkv_kernel(
    w_ref, cum_ref, state_ref, r_ref, k_ref, v_ref, dy_ref, u_ref, mid_ref, up_ref,
    proj_ref, part_ref, raise_ref, sums_ref,
):
    w, cumul = w_ref[...], cum_ref[...]
    before = cumul - w
    final = cumul[TOK - 1 : TOK]
    rb, kb, vb, dyb = r_ref[...], k_ref[...], v_ref[...], dy_ref[...]
    r, k, v, dy = (a.astype(F32) for a in (rb, kb, vb, dyb))
    u = u_ref[...]
    own = block_diagonal()
    odd = odd_rows()
    left = iota((COL, 128), 1) < 64
    packed = state_ref[...]
    state = jnp.where(left, packed, 0.0)
    grad = jnp.where(left, 0.0, packed)
    state = jnp.where(odd, pltpu.roll(state, 64, 1), state)
    grad = jnp.where(odd, grad, pltpu.roll(grad, 64, 1))
    state = jnp.where(own, jnp.concatenate([state, state], axis=1), 0.0)
    grad = jnp.where(own, jnp.concatenate([grad, grad], axis=1), 0.0)

    to_end = jnp.exp(jnp.minimum(final - cumul, 0.0))
    gr_mem = jnp.exp(before) * mm_left_exact(dyb, state, LANES_LANES)
    gk_out = to_end * mm_left_exact(vb, grad, LANES_LANES)
    gv = mm3(k * to_end, grad)
    across = mm_left_exact(jnp.ones((8, COL), BF16), state * grad, LANES_LANES, 3)[0:1] * jnp.exp(final)

    lane_head = head_of(iota((TOK, COL), 1))
    heads = [lane_head == h for h in range(4)]
    zero16 = jnp.zeros((TOK, COL), BF16)

    def by_head(a):
        return jnp.concatenate([jnp.where(m, a, zero16) for m in heads], axis=0)

    v_heads, dy_heads = by_head(vb), by_head(dyb)
    pair_ts = mm(dy_heads, vb, LANES_LANES)
    pair_st = mm(v_heads, dyb, LANES_LANES)
    ts_top, ts_low = (lane_cat(p) for p in parts(pair_ts, 2))
    st_top, st_low = (lane_cat(p) for p in parts(pair_st, 2))

    def wide_mm(top, low, mask, factor):
        f_top, f_low = (by_head(p) for p in parts(factor, 2))
        zero = jnp.zeros((TOK, 4 * TOK), BF16)
        top, low = jnp.where(mask, top, zero), jnp.where(mask, low, zero)
        return mm(top, f_top) + (mm(top, f_low) + mm(low, f_top))

    gk_in = jnp.zeros((TOK, COL), F32)
    score_st = jnp.zeros((4 * TOK, TOK), F32)
    tok = iota((TOK, COL), 0)
    for half in (64, 32, 16, 8):
        size = 2 * half
        second = (tok % size) >= half
        middle = cumul.reshape(TOK // size, size, COL)[:, half - 1 : half]
        middle = jnp.broadcast_to(middle, (TOK // size, size, COL)).reshape(TOK, COL)
        fade = jnp.exp(jnp.minimum(jnp.where(second, before - middle, middle - cumul), 0.0))
        late, early = jnp.where(second, fade, 0.0), jnp.where(second, 0.0, fade)
        r_hat, k_hat = r * late, k * early
        block_row = iota((TOK, 4 * TOK), 0) // size
        block_col = (iota((TOK, 4 * TOK), 1) % TOK) // size
        same = block_row == block_col
        gr_mem = gr_mem + late * wide_mm(ts_top, ts_low, same, k_hat)
        gk_in = gk_in + early * wide_mm(st_top, st_low, same, r_hat)
        k_top, k_low = (by_head(p) for p in parts(k_hat, 2))
        r_top, r_low = parts(r_hat, 2)
        score = mm(k_top, r_top, LANES_LANES) + (mm(k_top, r_low, LANES_LANES) + mm(k_low, r_top, LANES_LANES))
        same_st = ((iota((4 * TOK, TOK), 0) % TOK) // size) == (iota((4 * TOK, TOK), 1) // size)
        score_st = score_st + jnp.where(same_st, score, 0.0)
    for piece in parts(score_st, 2):
        gv = gv + mm(lane_cat(piece), dy_heads)

    spread = jnp.where(own, 1.0, 0.0).astype(BF16)

    def tiles(a):
        return a.reshape(TOK // 8, 8, COL)

    def flat(a):
        return a.reshape(TOK, COL)

    sub = iota((TOK // 8, 8, COL), 1)
    for d in range(1, 8):
        valid = sub >= d
        cum_old = pltpu.roll(tiles(cumul), d, 1)
        k_old = pltpu.roll(tiles(k), d, 1)
        v_old = pltpu.roll(tiles(v), d, 1)
        fade = jnp.exp(jnp.minimum(jnp.where(valid, tiles(before) - cum_old, 0.0), 0.0))
        fade = flat(jnp.where(valid, fade, 0.0))
        pair = mm_right_exact(dy * flat(v_old), spread)
        faded_r = fade * r
        gr_mem = gr_mem + fade * pair * flat(k_old)
        gk_in = gk_in + flat(pltpu.roll(tiles(faded_r * pair), 8 - d, 1))
        score = mm_right_exact(faded_r * flat(k_old), spread)
        gv = gv + flat(pltpu.roll(tiles(score * dy), 8 - d, 1))

    self_pair = mm_right_exact(dy * v, spread)
    self_score = mm_right_exact(r * u * k, spread)
    gv = gv + self_score * dy
    r_pair = r * self_pair
    proj_ref[0] = (gr_mem + u * k * self_pair).astype(BF16)
    proj_ref[1] = (gk_in + gk_out + u * r_pair).astype(BF16)
    proj_ref[2] = gv.astype(BF16)

    k_in = k * gk_in
    g_log = across - k_in + mm_left_exact(lower_ones(True), k * gk_out)
    g_log = g_log + mm_left_exact(upper_ones(), r * gr_mem - k_in)
    g_pre = g_log * w
    part_ref[...] = mm3(g_pre, up_ref[...], LANES_LANES).reshape(N_HEAD, 8, 128)
    raise_ref[...] = mm3(mid_ref[...].T, g_pre)
    floor_row = jnp.sum(g_pre, axis=0, keepdims=True)
    bonus_row = jnp.sum(k * r_pair, axis=0, keepdims=True)
    row = iota((8, COL), 0)
    sums_ref[...] = jnp.where(row == 0, floor_row, jnp.where(row == 1, bonus_row, 0.0))


def wkv_grads(w, cumul, state, r, k, v, dy, u, mid, up):
    return pl.pallas_call(
        wkv_kernel,
        out_shape=(
            jax.ShapeDtypeStruct((3, TOK, COL), BF16),
            jax.ShapeDtypeStruct((N_HEAD, 8, 128), F32),
            jax.ShapeDtypeStruct((RANK, COL), F32),
            jax.ShapeDtypeStruct((8, COL), F32),
        ),
        in_specs=[VMEM] * 10,
        out_specs=(VMEM,) * 4,
        cost_estimate=pl.CostEstimate(flops=10**10, bytes_accessed=10**6, transcendentals=0),
        name="wkv_grads",
    )(w, cumul, state, r, k, v, dy, u, mid, up)


def adapter_out_kernel(
    part_ref, proj_ref, mid_out, both_ref,
    land, full, send1, recv1, send2, recv2, swap_send, swap_recv, near_send, near_recv, edge_in, far_send, far_recv,
):
    h, s = lax.axis_index("head"), lax.axis_index("seq")
    core = h % 2
    mate = h + 1 - 2 * core
    after, ahead = (s + 1) % N_SEQ, (s + N_SEQ - 1) % N_SEQ
    barrier = pltpu.get_barrier_semaphore()
    loop(1, N_HEAD, lambda d: greet(barrier, {"head": (h + d) % N_HEAD}))
    for other in (after, ahead):
        greet(barrier, {"seq": other})
        greet(barrier, {"seq": other, "head": mate})
    pl.semaphore_wait(barrier, N_HEAD + 3)
    swap = remote(proj_ref, both_ref.at[core, :, pl.ds(0, TOK)], swap_send, swap_recv, {"head": mate})
    swap.start()
    edge = proj_ref.at[:, pl.ds(0, 16)]
    near = remote(edge, edge_in.at[core], near_send, near_recv, {"seq": ahead})
    far = remote(edge, edge_in.at[core], far_send, far_recv, {"seq": ahead, "head": mate})
    near.start()
    far.start()
    both_ref[core, :, pl.ds(0, TOK)] = proj_ref[...]
    finish = head_total(h, part_ref, land, full, (send1, recv1, send2, recv2))
    near.wait()
    far.wait()
    last = s == N_SEQ - 1
    both_ref[:, :, pl.ds(TOK, 16)] = jnp.where(last, jnp.zeros((2, 3, 16, COL), BF16), edge_in[...])
    finish()
    mid_out[...] = full[...].reshape(TOK, RANK)
    swap.wait()


def adapter_out(part, proj):
    return pl.pallas_call(
        adapter_out_kernel,
        out_shape=(
            jax.ShapeDtypeStruct((TOK, RANK), F32),
            jax.ShapeDtypeStruct((2, 3, TOK + 16, COL), BF16),
        ),
        in_specs=[VMEM] * 2,
        out_specs=(VMEM, VMEM),
        scratch_shapes=[
            *HEAD_SCRATCH[1:],
            *[pltpu.SemaphoreType.DMA] * 4,
            pltpu.VMEM((2, 3, 16, COL), BF16),
            *[pltpu.SemaphoreType.DMA] * 2,
        ],
        compiler_params=comm_params(2),
        cost_estimate=pl.CostEstimate(flops=10**10, bytes_accessed=10**6, transcendentals=0),
        name="adapter_out",
    )(part, proj)


def adapter_grads_kernel(raw_ref, mid_ref, x_ref, row_ref, mix_ref, down_ref, raise_ref, sums_ref, gdi_ref, big_ref):
    mid = mid_ref[...]
    g_mid = raw_ref[...] * (1.0 - mid * mid)
    down_t = down_ref[...]
    gdi_ref[...] = mm3(g_mid, down_t, LANES_LANES)
    decay_in = shift_mix(x_ref[...].astype(F32), row_ref[0:1], mix_ref[...])
    big_ref[0:16, 0:16] = mm3(decay_in.T, g_mid).reshape(16, 16, 128)
    big_ref[16:24, 0:16] = raise_ref[:, 0:128].reshape(8, 16, 128)
    big_ref[24:32, 0:16] = raise_ref[:, 128:256].reshape(8, 16, 128)
    sums = sums_ref[...]
    small = jnp.where(iota((8, 128), 0) < 2, sums[:, 0:128], pltpu.roll(sums[:, 128:256], 2, 0))
    big_ref[:, 16:24] = jnp.broadcast_to(small[None], (N_SEQ, 8, 128))


def adapter_grads(raw, mid, x, row, mix, down, raising, sums):
    return pl.pallas_call(
        adapter_grads_kernel,
        out_shape=(
            jax.ShapeDtypeStruct((TOK, COL), F32),
            jax.ShapeDtypeStruct((N_SEQ, 24, 128), F32),
        ),
        in_specs=[VMEM] * 8,
        out_specs=(VMEM, VMEM),
        cost_estimate=pl.CostEstimate(flops=10**9, bytes_accessed=10**6, transcendentals=0),
        name="adapter_grads",
    )(raw, mid, x, row, mix, down, raising, sums)


def project_kernel(both_ref, w_ref, mix_ref, out_ref):
    own = jnp.zeros((TOK, 128), F32)
    prior = jnp.zeros((TOK + 16, 128), F32)
    mixes = mix_ref[0]
    for m in range(3):
        weights = w_ref[:, m].reshape(128, 2 * COL)
        term = mm(both_ref[0, m], weights[:, :COL], LANES_LANES) + mm(both_ref[1, m], weights[:, COL:], LANES_LANES)
        mix = mixes[m : m + 1]
        own = own + (1.0 - mix) * term[:TOK]
        prior = prior + mix * term
    out_ref[0] = (own + pltpu.roll(prior, TOK + 15, 0)[:TOK]).astype(BF16)


def project(both, weights, mixes):
    return pl.pallas_call(
        project_kernel,
        grid=(N_HEAD,),
        out_shape=jax.ShapeDtypeStruct((N_HEAD, TOK, 128), BF16),
        in_specs=[
            pl.BlockSpec((2, 3, TOK + 16, COL), lambda i: (0, 0, 0, 0)),
            pl.BlockSpec((2, 3, 64, 2 * COL), lambda i: (i, 0, 0, 0)),
            pl.BlockSpec((1, 8, 128), lambda i: (i, 0, 0)),
        ],
        out_specs=pl.BlockSpec((1, TOK, 128), lambda i: (i, 0, 0)),
        cost_estimate=pl.CostEstimate(flops=10**10, bytes_accessed=10**7, transcendentals=0),
        name="project",
    )(both, weights, mixes)


def last_kernel(
    y_ref, big_ref, gdi_ref, mix_ref, out_ref, down_ref, raise_ref, small_ref,
    y_in, big_in, total, edge, y_send, y_recv, send1, recv1, send2, recv2, e_send, e_recv,
):
    h, s = lax.axis_index("head"), lax.axis_index("seq")
    after, ahead = (s + 1) % N_SEQ, (s + N_SEQ - 1) % N_SEQ
    barrier = pltpu.get_barrier_semaphore()
    loop(1, N_HEAD, lambda d: greet(barrier, {"head": (h + d) % N_HEAD}))
    loop(1, N_SEQ, lambda d: greet(barrier, {"seq": (s + d) % N_SEQ}))
    pl.semaphore_wait(barrier, N_HEAD + N_SEQ - 2)

    def y_out(d):
        to = (h + d) % N_HEAD
        return remote(y_ref.at[to], y_in.at[h], y_send.at[to], y_recv.at[h], {"head": to})

    def y_from(d):
        frm = (h + d) % N_HEAD
        return remote(y_ref.at[frm], y_in.at[frm], y_send.at[frm], y_recv.at[frm], {"head": frm})

    def first(d):
        to = (s + d) % N_SEQ
        return remote(big_ref.at[to], big_in.at[s], send1.at[to], recv1.at[s], {"seq": to})

    def first_in(d):
        frm = (s + d) % N_SEQ
        return remote(big_ref.at[frm], big_in.at[frm], send1.at[frm], recv1.at[frm], {"seq": frm})

    def second(d):
        to = (s + d) % N_SEQ
        return remote(total.at[s], total.at[s], send2.at[to], recv2.at[s], {"seq": to})

    def second_in(d):
        frm = (s + d) % N_SEQ
        return remote(total.at[frm], total.at[frm], send2.at[frm], recv2.at[frm], {"seq": frm})

    loop(1, N_SEQ, lambda d: first(d).start())
    loop(1, N_HEAD, lambda d: y_out(d).start())
    row_copy = remote(gdi_ref.at[pl.ds(0, 8)], edge, e_send, e_recv, {"seq": ahead})
    row_copy.start()
    big_in[s] = big_ref[s]
    y_in[h] = y_ref[h]
    loop(1, N_SEQ, lambda d: first_in(d).wait_recv())
    acc = big_in[0]
    for n in range(1, N_SEQ):
        acc = acc + big_in[n]
    total[s] = acc[:16]
    loop(1, N_SEQ, lambda d: second(d).start())
    small_ref[...] = acc[16:24]
    row_copy.wait()
    gdi = gdi_ref[...]
    next_row = jnp.where(s == N_SEQ - 1, 0.0, edge[0:1])
    shifted = jnp.where(iota((TOK, COL), 0) == TOK - 1, next_row, pltpu.roll(gdi, TOK - 1, 0))
    mix = mix_ref[...]
    mine = (1.0 - mix) * gdi + mix * shifted
    loop(1, N_HEAD, lambda d: y_from(d).wait_recv())
    halves = []
    for core in range(2):
        acc = y_in[core].astype(F32)
        for y in range(1, 8):
            acc = acc + y_in[2 * y + core].astype(F32)
        halves.append(acc)
    low = iota((TOK, 128), 1) < 64
    even = jnp.where(low, halves[0], pltpu.roll(halves[1], 64, 1))
    odd = jnp.where(low, pltpu.roll(halves[0], 64, 1), halves[1])
    out_ref[:, 0:128] = (even + mine[:, 0:128]).astype(BF16)
    out_ref[:, 128:256] = (odd + mine[:, 128:256]).astype(BF16)
    loop(1, N_SEQ, lambda d: second_in(d).wait_recv())
    down_ref[...] = total[0:16].reshape(COL, RANK)
    raise_ref[:, 0:128] = total[16:24].reshape(RANK, 128)
    raise_ref[:, 128:256] = total[24:32].reshape(RANK, 128)
    loop(1, N_HEAD, lambda d: y_from(d).wait_send())
    loop(1, N_SEQ, lambda d: first_in(d).wait_send())
    loop(1, N_SEQ, lambda d: second_in(d).wait_send())


def last(y, big, gdi, mix):
    return pl.pallas_call(
        last_kernel,
        out_shape=(
            jax.ShapeDtypeStruct((TOK, COL), BF16),
            jax.ShapeDtypeStruct((COL, RANK), F32),
            jax.ShapeDtypeStruct((RANK, COL), F32),
            jax.ShapeDtypeStruct((8, 128), F32),
        ),
        in_specs=[VMEM] * 4,
        out_specs=(VMEM,) * 4,
        scratch_shapes=[
            pltpu.VMEM((N_HEAD, TOK, 128), BF16),
            pltpu.VMEM((N_SEQ, 24, 128), F32),
            pltpu.VMEM((N_SEQ, 16, 128), F32),
            pltpu.VMEM((8, COL), F32),
            *[pltpu.SemaphoreType.DMA((N_HEAD,))] * 2,
            *[pltpu.SemaphoreType.DMA((N_SEQ,))] * 4,
            *[pltpu.SemaphoreType.DMA] * 2,
        ],
        compiler_params=comm_params(3),
        cost_estimate=pl.CostEstimate(flops=10**10, bytes_accessed=10**6, transcendentals=0),
        name="last",
    )(y, big, gdi, mix)


def gathered_weights(proj_weights):
    head = lax.axis_index("head")
    core = head % 2
    keep = lax.dynamic_slice_in_dim(proj_weights, core * 64, 64, 1)
    give = lax.dynamic_slice_in_dim(proj_weights, (1 - core) * 64, 64, 1)
    taken = lax.ppermute(give, "head", [(i, i ^ 1) for i in range(N_HEAD)])
    first = core == 0
    mine = jnp.concatenate([jnp.where(first, keep, taken), jnp.where(first, taken, keep)], axis=2)
    return lax.all_gather(mine, "seq")


def per_device(
    layer_input, receptance, key_act, value_act, attention_result_sensitivity, time_first,
    decay_exponent_base, decay_shift_mix, mix_rkv, decay_adapter_down, decay_adapter_up, proj_weights,
):
    weights = gathered_weights(proj_weights)
    core = lax.axis_index("head") % 2
    mixes = lax.dynamic_index_in_dim(mix_rkv.reshape(3, N_HEAD, 2, 2, 64), core, 3, keepdims=False)
    mixes = jnp.moveaxis(mixes.reshape(3, N_HEAD, 128), 0, 1)
    mixes = jnp.pad(mixes, ((0, 0), (0, 5), (0, 0)))
    mix = decay_shift_mix[None]
    u = time_first.reshape(1, COL)
    acts = (receptance, key_act, value_act, attention_result_sensitivity)
    pre, row = adapter_in(layer_input, mix, decay_adapter_down)
    mid, w, cumul, pack = local_terms(pre, decay_exponent_base[None], decay_adapter_up, *acts)
    state = state_exchange(pack)
    proj, part, raising, sums = wkv_grads(w, cumul, state, *acts, u, mid, decay_adapter_up)
    raw, both = adapter_out(part, proj)
    gdi, big = adapter_grads(raw, mid, layer_input, row, mix, decay_adapter_down, raising, sums)
    y = project(both, weights, mixes)
    out, down_grad, up_grad, small = last(y, big, gdi, mix)
    base_grad = jnp.concatenate([small[0], small[2]])
    bonus_grad = jnp.concatenate([small[1], small[3]]).reshape(4, HS)
    return out, down_grad, up_grad, base_grad, bonus_grad


def solution(mesh):
    return jax.shard_map(
        per_device,
        mesh=mesh,
        in_specs=(
            P("seq", "head"), P("seq", "head"), P("seq", "head"), P("seq", "head"), P("seq", "head"),
            P("head", None), P("head"), P("head"), P(), P("head", None), P(None, "head"),
            P(None, "seq", "head"),
        ),
        out_specs=(P("seq", "head"), P("head", None), P(None, "head"), P("head"), P("head", None)),
        check_vma=False,
    )
```

```python
from types import SimpleNamespace

import jax
import jax.numpy as jnp
from jax import lax
from jax.experimental import pallas as pl
from jax.experimental.pallas import tpu as pltpu
from jax.sharding import PartitionSpec as P

F32 = jnp.float32
BF16 = jnp.bfloat16
MESH = pl.DeviceIdType.MESH
N_HEAD = 16
N_SEQ = 32
TOK = 128
COL = 256
HS = 64
RANK = 128
VMEM = pl.BlockSpec(memory_space=pltpu.VMEM)

ROWS_LANES = (((1,), (0,)), ((), ()))
LANES_LANES = (((1,), (1,)), ((), ()))


def mm(a, b, dims=ROWS_LANES):
    return lax.dot_general(a, b, dims, preferred_element_type=F32)


def parts(a, count):
    out = []
    for _ in range(count - 1):
        top = a.astype(BF16)
        out.append(top)
        a = a - top.astype(F32)
    out.append(a.astype(BF16))
    return out


def mm3(a, b, dims=ROWS_LANES):
    ah, al = parts(a, 2)
    bh, bl = parts(b, 2)
    return mm(ah, bh, dims) + (mm(ah, bl, dims) + mm(al, bh, dims))


def mm_right_exact(a, b, dims=ROWS_LANES, count=2):
    out = None
    for piece in parts(a, count):
        term = mm(piece, b, dims)
        out = term if out is None else out + term
    return out


def mm_left_exact(a, b, dims=ROWS_LANES, count=2):
    out = None
    for piece in parts(b, count):
        term = mm(a, piece, dims)
        out = term if out is None else out + term
    return out


def iota(shape, dim):
    return lax.broadcasted_iota(jnp.int32, shape, dim)


def head_of(index):
    return index // HS


def lower_ones(strict):
    row, col = iota((TOK, TOK), 0), iota((TOK, TOK), 1)
    keep = row > col if strict else row >= col
    return jnp.where(keep, 1.0, 0.0).astype(BF16)


def upper_ones():
    row, col = iota((TOK, TOK), 0), iota((TOK, TOK), 1)
    return jnp.where(row < col, 1.0, 0.0).astype(BF16)


def block_diagonal():
    return head_of(iota((COL, COL), 0)) == head_of(iota((COL, COL), 1))


def odd_rows():
    return (head_of(iota((COL, 128), 0)) % 2) == 1


def remote(src, dst, send_sem, recv_sem, to):
    return pltpu.make_async_remote_copy(
        src_ref=src, dst_ref=dst, send_sem=send_sem, recv_sem=recv_sem,
        device_id=to, device_id_type=MESH,
    )


def greet(barrier, to):
    pl.semaphore_signal(barrier, inc=1, device_id=to, device_id_type=MESH)


def loop(start, stop, body):
    def step(i, carry):
        body(i)
        return carry

    lax.fori_loop(start, stop, step, 0)


def shift_mix(x, carried, mix):
    previous = pltpu.roll(x, 1, 0)
    previous = jnp.where(iota((TOK, COL), 0) == 0, carried, previous)
    return x + mix * (previous - x)


class AllToAll:
    def __init__(self, axis, size, me, out, land, send, recv, broadcast=False):
        self.axis, self.size, self.me = axis, size, me
        self.out, self.land, self.send, self.recv, self.broadcast = out, land, send, recv, broadcast

    def _to(self, peer):
        src = self.out.at[self.me if self.broadcast else peer]
        return remote(src, self.land.at[self.me], self.send.at[peer], self.recv.at[self.me], {self.axis: peer})

    def _from(self, peer):
        src = self.out.at[self.me if self.broadcast else peer]
        return remote(src, self.land.at[peer], self.send.at[peer], self.recv.at[peer], {self.axis: peer})

    def _each(self, act):
        loop(1, self.size, lambda d: act((self.me + d) % self.size))

    def start(self):
        self._each(lambda p: self._to(p).start())

    def wait_recv(self):
        self._each(lambda p: self._from(p).wait_recv())

    def wait_send(self):
        self._each(lambda p: self._from(p).wait_send())


class WeightGather:
    def __init__(self, g, h, s):
        self.g = g
        self.core = h % 2
        self.mate = h + 1 - 2 * self.core
        self.pair = h - self.core
        self.x, self.z = s // 8, s % 8

    def seq(self, x, z):
        return x * 8 + z

    def zz(self, d):
        return (self.z + d + 8) % 8

    def xx(self, d):
        return (self.x + d + 4) % 4

    def half(self, c):
        return self.g.w.at[:, pl.ds(pl.multiple_of(c * 64, 64), 64)]

    def arrived(self, x, z, src):
        slot = self.g.buf.at[x, z, src]
        remote(slot, slot, self.g.mate_send, self.g.wrecv.at[x, z, src], {"head": self.mate}).wait_recv()

    def forward(self, x, z, src, way, act):
        slot = self.g.buf.at[x, z, src]
        place = (
            self.seq(self.x, self.zz(1)), self.seq(self.x, self.zz(-1)),
            self.seq(self.xx(1), self.z), self.seq(self.xx(-1), self.z),
        )[way]
        copy = remote(slot, slot, self.g.wsend.at[way, x, z, src], self.g.wrecv.at[x, z, src], {"seq": place})
        act(copy)

    def sources(self, act):
        g, core = self.g, self.core
        dst = g.buf.at[self.x, self.z, core]
        act(remote(self.half(1 - core), dst, g.mate_send, g.wrecv.at[self.x, self.z, core], {"head": self.mate}))

        @pl.when(core == 0)
        def _():
            for d in (1, 3, 2):
                place = self.seq(self.xx(d), self.z)
                for c in range(2):
                    act(remote(self.half(c), g.buf.at[self.x, self.z, 0], g.first_send.at[d, c],
                               g.wrecv.at[self.x, self.z, 0], {"seq": place, "head": self.pair + c}))

        @pl.when(core == 1)
        def _():
            for d in (1, 3):
                place = self.seq(self.x, self.zz(1 if d == 1 else -1))
                for c in range(2):
                    act(remote(self.half(c), g.buf.at[self.x, self.z, 1], g.first_send.at[d, c],
                               g.wrecv.at[self.x, self.z, 1], {"seq": place, "head": self.pair + c}))

    def keep_own(self):
        self.g.buf[self.x, self.z, self.core] = self.g.w[:, pl.ds(pl.multiple_of(self.core * 64, 64), 64)]

    def round_z0(self, d, act):
        if d < 3:
            for i in range(4):
                self.forward(i, self.zz(-d), 0, 0, act)
                self.forward(i, self.zz(d), 0, 1, act)
        else:
            for i in range(2):
                self.forward(i, self.zz(-d), 0, 0, act)
                self.forward(i + 2, self.zz(d), 0, 1, act)

    def round_z1(self, d, act):
        self.forward(self.x, self.zz(-d), 1, 0, act)
        if d < 3:
            self.forward(self.x, self.zz(d), 1, 1, act)

    def round_x1(self, z, act):
        self.forward(self.x, z, 1, 2, act)
        self.forward(self.x, z, 1, 3, act)

    def turn_x1(self, z, act):
        even = z % 2 == 0

        @pl.when(even)
        def _():
            self.forward(self.xx(-1), z, 1, 2, act)

        @pl.when(jnp.logical_not(even))
        def _():
            self.forward(self.xx(1), z, 1, 3, act)

    def wait_z0(self, d):
        for i in range(4):
            self.arrived(i, self.zz(d), 0)

    def wait_sides(self, z):
        self.arrived(self.xx(1), z, 1)
        self.arrived(self.xx(-1), z, 1)

    def stage(self, number):
        begin = lambda copy: copy.start()
        if number == 0:
            self.sources(begin)
            self.keep_own()
        if number == 1:
            for d in (1, 2, 3):
                self.arrived(self.xx(d), self.z, 0)
            self.arrived(self.x, self.z, 1 - self.core)
            self.round_z0(0, begin)
            self.round_x1(self.z, begin)
            for d in (-1, 1):
                self.arrived(self.x, self.zz(d), 1)
            self.round_z1(1, begin)
            for d in (-1, 1):
                self.round_x1(self.zz(d), begin)
        if number == 2:
            for d in (-1, 1):
                self.wait_z0(d)
            self.round_z0(1, begin)
            for d in (-2, 2):
                self.arrived(self.x, self.zz(d), 1)
            self.round_z1(2, begin)
            for d in (0, -1, 1):
                self.wait_sides(self.zz(d))
                self.turn_x1(self.zz(d), begin)
            for d in (-2, 2):
                self.round_x1(self.zz(d), begin)
        if number == 3:
            for d in (-2, 2):
                self.wait_z0(d)
            self.round_z0(2, begin)
            for d in (-3, 3):
                self.arrived(self.x, self.zz(d), 1)
            self.round_z1(3, begin)
            for d in (-2, 2):
                self.wait_sides(self.zz(d))
                self.turn_x1(self.zz(d), begin)
            for d in (-3, 3):
                self.round_x1(self.zz(d), begin)
        if number == 4:
            for d in (-3, 3):
                self.wait_z0(d)
            self.round_z0(3, begin)
            self.arrived(self.x, self.zz(4), 1)
            self.round_x1(self.zz(4), begin)
            for d in (-3, 3):
                self.wait_sides(self.zz(d))
                self.turn_x1(self.zz(d), begin)
        if number == 5:
            self.wait_z0(4)
            self.wait_sides(self.zz(4))
            self.turn_x1(self.zz(4), begin)

    def far_side(self, z):
        self.arrived(self.xx(2), z, 1)

    def wait_send(self):
        done = lambda copy: copy.wait_send()
        self.sources(done)
        for d in range(4):
            self.round_z0(d, done)
        for d in (1, 2, 3):
            self.round_z1(d, done)
        for d in range(8):
            self.round_x1(self.zz(d), done)
            self.turn_x1(self.zz(d), done)


INPUTS = ("x", "mix", "down", "base", "up", "r", "k", "v", "dy", "u", "w", "mixes")
OUTPUTS = {
    "out": ((TOK, COL), BF16),
    "down_grad": ((COL, RANK), F32),
    "up_grad": ((RANK, COL), F32),
    "base_grad": ((1, COL), F32),
    "bonus_grad": ((1, COL), F32),
}
DMA = pltpu.SemaphoreType.DMA
SCRATCH = {
    "part1": pltpu.VMEM((N_HEAD, 8, 128), F32),
    "land1": pltpu.VMEM((N_HEAD, 8, 128), F32),
    "full1": pltpu.VMEM((N_HEAD, 8, 128), F32),
    "part2": pltpu.VMEM((N_HEAD, 8, 128), F32),
    "land2": pltpu.VMEM((N_HEAD, 8, 128), F32),
    "full2": pltpu.VMEM((N_HEAD, 8, 128), F32),
    "edge_part": pltpu.VMEM((8, 128), F32),
    "edge_land": pltpu.VMEM((N_HEAD, 8, 128), F32),
    "tail": pltpu.VMEM((16, COL), BF16),
    "pack": pltpu.VMEM((N_SEQ, 2, 8, 128), F32),
    "pack_in": pltpu.VMEM((N_SEQ, 2, 8, 128), F32),
    "back": pltpu.VMEM((N_SEQ, 8, 128), F32),
    "got": pltpu.VMEM((N_SEQ, 8, 128), F32),
    "pairs": pltpu.VMEM((8, TOK, COL), F32),
    "cross": pltpu.VMEM((4, TOK, 4 * TOK), BF16),
    "hold": pltpu.VMEM((8, TOK, COL), F32),
    "proj": pltpu.VMEM((2, 3, TOK, COL), BF16),
    "proj_edge": pltpu.VMEM((2, 3, 16, COL), BF16),
    "turned": pltpu.VMEM((2, 3, COL, 2 * TOK), BF16),
    "big": pltpu.VMEM((N_SEQ, 24, 128), F32),
    "big_in": pltpu.VMEM((N_SEQ, 24, 128), F32),
    "total": pltpu.VMEM((N_SEQ, 16, 128), F32),
    "gdi": pltpu.VMEM((TOK, COL), F32),
    "gdi_edge": pltpu.VMEM((8, COL), F32),
    "y_out": pltpu.VMEM((N_HEAD, 128, TOK), BF16),
    "y_in": pltpu.VMEM((N_HEAD, 128, TOK), BF16),
    "buf": pltpu.VMEM((4, 8, 2, 3, 64, COL), BF16),
    "h_sems": DMA((9, N_HEAD)),
    "y_sems": DMA((2, N_HEAD)),
    "s_sems": DMA((8, N_SEQ)),
    "one": DMA((11,)),
    "wrecv": DMA((4, 8, 2)),
    "wsend": DMA((4, 4, 8, 2)),
    "first_send": DMA((4, 2)),
    "mate_send": DMA,
}


def step_kernel(*refs):
    g = SimpleNamespace(**dict(zip((*INPUTS, *OUTPUTS, *SCRATCH), refs, strict=True)))
    h, s = lax.axis_index("head"), lax.axis_index("seq")
    core = h % 2
    mate = h + 1 - 2 * core
    nxt, prv = (s + 1) % N_SEQ, (s + N_SEQ - 1) % N_SEQ
    weights = WeightGather(g, h, s)

    barrier = pltpu.get_barrier_semaphore()
    loop(1, N_HEAD, lambda d: greet(barrier, {"head": (h + d) % N_HEAD}))

    def greet_seq(d):
        greet(barrier, {"seq": (s + d) % N_SEQ})
        greet(barrier, {"seq": (s + d) % N_SEQ, "head": mate})

    loop(1, N_SEQ, greet_seq)

    @pl.when(h == 0)
    def _():
        loop(0, N_HEAD, lambda j: greet(barrier, {"seq": prv, "head": j}))

    pl.semaphore_wait(barrier, N_HEAD - 1 + 2 * (N_SEQ - 1) + 1)

    row_copy = remote(g.x.at[pl.ds(TOK - 16, 16)], g.tail, g.one.at[0], g.one.at[1], {"seq": nxt})
    row_copy.start()
    x = g.x[...].astype(F32)
    mix = g.mix[...]
    down_h, down_l = parts(g.down[...], 2)

    def into_rank(a):
        a_h, a_l = parts(a, 2)
        return mm(a_h, down_h) + (mm(a_h, down_l) + mm(a_l, down_h))

    g.part1[...] = into_rank(shift_mix(x, 0.0, mix)).reshape(N_HEAD, 8, 128)
    in_first = AllToAll("head", N_HEAD, h, g.part1, g.land1, g.h_sems.at[0], g.h_sems.at[1])
    in_first.start()
    g.edge_part[...] = into_rank(mix * x[TOK - 8 :])
    edge_copy = remote(g.edge_part, g.edge_land.at[h], g.one.at[2], g.h_sems.at[4, h], {"seq": nxt, "head": 0})
    edge_copy.start()
    weights.stage(0)

    rb, kb, vb, dyb = g.r[...], g.k[...], g.v[...], g.dy[...]
    r, k, v, dy = (a.astype(F32) for a in (rb, kb, vb, dyb))
    u = g.u[...]
    own = block_diagonal()
    odd = odd_rows()
    lane_head = head_of(iota((TOK, COL), 1))
    heads = [lane_head == i for i in range(4)]
    zero16 = jnp.zeros((TOK, COL), BF16)

    def by_head(a):
        return jnp.concatenate([jnp.where(m, a, zero16) for m in heads], axis=0)

    def lane_cat(stacked):
        return jnp.concatenate([stacked[i * TOK : (i + 1) * TOK] for i in range(4)], axis=1)

    spread = jnp.where(own, 1.0, 0.0).astype(BF16)

    def tiles(a):
        return a.reshape(TOK // 8, 8, COL)

    def flat(a):
        return a.reshape(TOK, COL)

    for i, piece in enumerate(parts(mm(by_head(dyb), vb, LANES_LANES), 2)):
        g.cross[i] = lane_cat(piece)
    for i, piece in enumerate(parts(mm(by_head(vb), dyb, LANES_LANES), 2)):
        g.cross[2 + i] = lane_cat(piece)
    for d in range(8):
        v_old = v if d == 0 else flat(pltpu.roll(tiles(v), d, 1))
        g.pairs[d] = mm_right_exact(dy * v_old, spread)

    g.land1[h] = g.part1[h]
    in_first.wait_recv()

    @pl.when(h == 0)
    def _():
        def got_edge(j):
            remote(g.edge_part, g.edge_land.at[j], g.one.at[2], g.h_sems.at[4, j], {"seq": nxt}).wait_recv()

        loop(0, N_HEAD, got_edge)
        rows = g.edge_land[0]
        for j in range(1, N_HEAD):
            rows = rows + g.edge_land[j]
        first_row = jnp.where((iota((8, 128), 0) == 0) & (s > 0), pltpu.roll(rows, 1, 0), 0.0)
        g.land1[0] = g.land1[0] + first_row

    def summed(ref):
        acc = ref[0]
        for j in range(1, N_HEAD):
            acc = acc + ref[j]
        return acc

    g.full1[h] = summed(g.land1)
    in_second = AllToAll("head", N_HEAD, h, g.full1, g.full1, g.h_sems.at[2], g.h_sems.at[3], True)
    in_second.start()
    weights.stage(1)
    in_second.wait_recv()

    mid = jnp.tanh(g.full1[...].reshape(TOK, RANK))
    up_h, up_l = parts(g.up[...], 2)
    mid_h, mid_l = parts(mid, 2)
    w = -jnp.exp(g.base[...] + (mm(mid_h, up_h) + (mm(mid_h, up_l) + mm(mid_l, up_h))))
    w_parts = parts(w, 3)
    ones = lower_ones(False)
    cumul = mm(ones, w_parts[0]) + (mm(ones, w_parts[1]) + mm(ones, w_parts[2]))
    before = cumul - w
    final = cumul[TOK - 1 : TOK]
    all_ones = jnp.ones((TOK, 128), BF16)
    w_turned = [p.astype(F32).T.astype(BF16) for p in w_parts]
    total_rows = mm(w_turned[0], all_ones) + (mm(w_turned[1], all_ones) + mm(w_turned[2], all_ones))
    to_end = jnp.exp(jnp.minimum(final - cumul, 0.0))
    from_start = jnp.exp(before)

    def folded(a, b):
        wide = jnp.where(own, mm_right_exact(a.T, b), 0.0)
        return wide[:, :128] + wide[:, 128:]

    state = folded(k * to_end, vb)
    grad = folded(r * from_start, dyb)
    packed = jnp.where(odd, pltpu.roll(state, 64, 1), state) + jnp.where(odd, grad, pltpu.roll(grad, 64, 1))
    g.pack[:, 0] = packed.reshape(N_SEQ, 8, 128)
    g.pack[:, 1] = jnp.exp(total_rows).reshape(N_SEQ, 8, 128)
    to_owner = AllToAll("seq", N_SEQ, s, g.pack, g.pack_in, g.s_sems.at[0], g.s_sems.at[1])
    to_owner.start()
    g.pack_in[s] = g.pack[s]
    g.hold[0], g.hold[1], g.hold[2], g.hold[3] = w, cumul, to_end, from_start

    gr_mem = jnp.zeros((TOK, COL), F32)
    gk_in = jnp.zeros((TOK, COL), F32)
    score_st = jnp.zeros((4 * TOK, TOK), F32)
    tok = iota((TOK, COL), 0)

    def wide_mm(first, mask, factor):
        f_top, f_low = (by_head(p) for p in parts(factor, 2))
        zero = jnp.zeros((TOK, 4 * TOK), BF16)
        top, low = jnp.where(mask, g.cross[first], zero), jnp.where(mask, g.cross[first + 1], zero)
        return mm(top, f_top) + (mm(top, f_low) + mm(low, f_top))

    for half in (64, 32, 16, 8):
        size = 2 * half
        second = (tok % size) >= half
        middle = cumul.reshape(TOK // size, size, COL)[:, half - 1 : half]
        middle = jnp.broadcast_to(middle, (TOK // size, size, COL)).reshape(TOK, COL)
        fade = jnp.exp(jnp.minimum(jnp.where(second, before - middle, middle - cumul), 0.0))
        late, early = jnp.where(second, fade, 0.0), jnp.where(second, 0.0, fade)
        r_hat, k_hat = r * late, k * early
        same = iota((TOK, 4 * TOK), 0) // size == (iota((TOK, 4 * TOK), 1) % TOK) // size
        gr_mem = gr_mem + late * wide_mm(0, same, k_hat)
        gk_in = gk_in + early * wide_mm(2, same, r_hat)
        k_top, k_low = (by_head(p) for p in parts(k_hat, 2))
        r_top, r_low = parts(r_hat, 2)
        score = mm(k_top, r_top, LANES_LANES) + (mm(k_top, r_low, LANES_LANES) + mm(k_low, r_top, LANES_LANES))
        same_st = (iota((4 * TOK, TOK), 0) % TOK) // size == iota((4 * TOK, TOK), 1) // size
        score_st = score_st + jnp.where(same_st, score, 0.0)
    gv = jnp.zeros((TOK, COL), F32)
    dy_heads = by_head(dyb)
    for piece in parts(score_st, 2):
        gv = gv + mm(lane_cat(piece), dy_heads)

    to_owner.wait_recv()
    onward = jnp.zeros((8, 128), F32)
    forward = []
    for n in range(N_SEQ):
        forward.append(onward)
        onward = g.pack_in[n, 1] * onward + g.pack_in[n, 0]
    left8 = iota((8, 128), 1) < 64
    reverse = jnp.zeros((8, 128), F32)
    for n in reversed(range(N_SEQ)):
        g.back[n] = jnp.where(left8, forward[n], reverse)
        reverse = g.pack_in[n, 1] * reverse + g.pack_in[n, 0]
    to_range = AllToAll("seq", N_SEQ, s, g.back, g.got, g.s_sems.at[2], g.s_sems.at[3])
    to_range.start()
    g.got[s] = g.back[s]
    weights.stage(2)

    sub = iota((TOK // 8, 8, COL), 1)
    for d in range(1, 8):
        valid = sub >= d
        cum_old = pltpu.roll(tiles(cumul), d, 1)
        k_old = flat(pltpu.roll(tiles(k), d, 1))
        fade = jnp.exp(jnp.minimum(jnp.where(valid, tiles(before) - cum_old, 0.0), 0.0))
        fade = flat(jnp.where(valid, fade, 0.0))
        pair = g.pairs[d]
        faded_r = fade * r
        gr_mem = gr_mem + fade * pair * k_old
        gk_in = gk_in + flat(pltpu.roll(tiles(faded_r * pair), 8 - d, 1))
        score = mm_right_exact(faded_r * k_old, spread)
        gv = gv + flat(pltpu.roll(tiles(score * dy), 8 - d, 1))
    gv = gv + mm_right_exact(r * u * k, spread) * dy
    g.hold[4], g.hold[5], g.hold[6] = gr_mem, gk_in, gv
    to_range.wait_recv()

    w, cumul, to_end, from_start = g.hold[0], g.hold[1], g.hold[2], g.hold[3]
    packed = g.got[...].reshape(COL, 128)
    left = iota((COL, 128), 1) < 64
    state, grad = jnp.where(left, packed, 0.0), jnp.where(left, 0.0, packed)
    state = jnp.where(odd, pltpu.roll(state, 64, 1), state)
    grad = jnp.where(odd, grad, pltpu.roll(grad, 64, 1))
    state = jnp.where(own, jnp.concatenate([state, state], axis=1), 0.0)
    grad = jnp.where(own, jnp.concatenate([grad, grad], axis=1), 0.0)
    gr_mem = g.hold[4] + from_start * mm_left_exact(dyb, state, LANES_LANES)
    gk_in = g.hold[5]
    gk_out = to_end * mm_left_exact(vb, grad, LANES_LANES)
    across = mm_left_exact(jnp.ones((8, COL), BF16), state * grad, LANES_LANES, 3)[0:1]
    across = across * jnp.exp(cumul[TOK - 1 : TOK])
    k_in = k * gk_in
    g_log = across - k_in + mm_left_exact(lower_ones(True), k * gk_out)
    g_log = g_log + mm_left_exact(upper_ones(), r * gr_mem - k_in)
    g_pre = g_log * w
    g.part2[...] = mm3(g_pre, g.up[...], LANES_LANES).reshape(N_HEAD, 8, 128)
    out_first = AllToAll("head", N_HEAD, h, g.part2, g.land2, g.h_sems.at[5], g.h_sems.at[6])
    out_first.start()
    g.land2[h] = g.part2[h]

    self_pair = g.pairs[0]
    r_pair = r * self_pair
    g.proj[core, 0] = (gr_mem + u * k * self_pair).astype(BF16)
    g.proj[core, 1] = (gk_in + gk_out + u * r_pair).astype(BF16)
    g.proj[core, 2] = (g.hold[6] + mm3(k * to_end, grad)).astype(BF16)
    swap = remote(g.proj.at[core], g.proj.at[core], g.one.at[3], g.one.at[4], {"head": mate})
    first_rows = g.proj.at[core, :, pl.ds(0, 16)]
    near = remote(first_rows, g.proj_edge.at[core], g.one.at[5], g.one.at[6], {"seq": prv})
    far = remote(first_rows, g.proj_edge.at[core], g.one.at[7], g.one.at[8], {"seq": prv, "head": mate})
    swap.start()
    near.start()
    far.start()
    weights.stage(3)
    raising = mm3(mid.T, g_pre)
    g.big[16:24, 0:16] = raising[:, 0:128].reshape(8, 16, 128)
    g.big[24:32, 0:16] = raising[:, 128:256].reshape(8, 16, 128)
    floor_row = jnp.sum(g_pre, axis=0, keepdims=True)
    bonus_row = jnp.sum(k * r_pair, axis=0, keepdims=True)
    row8 = iota((8, 128), 0)
    small = jnp.where(row8 == 0, floor_row[:, :128], 0.0) + jnp.where(row8 == 1, floor_row[:, 128:], 0.0)
    small = small + jnp.where(row8 == 2, bonus_row[:, :128], 0.0) + jnp.where(row8 == 3, bonus_row[:, 128:], 0.0)
    g.big[:, 16:24] = jnp.broadcast_to(small[None], (N_SEQ, 8, 128))
    row_copy.wait()
    carried = jnp.where(s == 0, 0.0, g.tail[...].astype(F32)[15:16])
    turned_in = shift_mix(x, carried, mix).T

    out_first.wait_recv()
    g.full2[h] = summed(g.land2)
    out_second = AllToAll("head", N_HEAD, h, g.full2, g.full2, g.h_sems.at[7], g.h_sems.at[8], True)
    out_second.start()

    swap.wait()
    near.wait()
    far.wait()
    for c in range(2):
        for m in range(3):
            a = g.proj[c, m].astype(F32)
            edge = jnp.where(s == N_SEQ - 1, 0.0, g.proj_edge[c, m].astype(F32)[0:1])
            later = jnp.where(tok == TOK - 1, edge, pltpu.roll(a, TOK - 1, 0))
            g.turned[c, m, :, 0:TOK] = a.T.astype(BF16)
            g.turned[c, m, :, TOK:] = later.T.astype(BF16)
    out_second.wait_recv()

    g_mid = g.full2[...].reshape(TOK, RANK) * (1.0 - mid * mid)
    g.big[0:16, 0:16] = mm3(turned_in, g_mid).reshape(16, 16, 128)
    sums_first = AllToAll("seq", N_SEQ, s, g.big, g.big_in, g.s_sems.at[4], g.s_sems.at[5])
    gdi = mm3(g_mid, g.down[...], LANES_LANES)
    g.gdi[...] = gdi
    edge_row = remote(g.gdi.at[pl.ds(0, 8)], g.gdi_edge, g.one.at[9], g.one.at[10], {"seq": prv})
    weights.stage(4)
    sums_first.start()
    edge_row.start()
    g.big_in[s] = g.big[s]

    def y_send(to):
        return remote(g.y_out.at[to], g.y_in.at[h], g.y_sems.at[0, to], g.y_sems.at[1, h], {"head": to})

    def y_from(frm):
        return remote(g.y_out.at[frm], g.y_in.at[frm], g.y_sems.at[0, frm], g.y_sems.at[1, frm], {"head": frm})

    near_pair = (s % 8) // 2
    for turn in (0, 1, 3, 2):
        pair = (near_pair + turn) % 4
        if turn == 2:
            weights.stage(5)
        weights.far_side(2 * pair)
        weights.far_side(2 * pair + 1)
        mixes = g.mixes[pair].T
        acc = jnp.zeros((4 * TOK, TOK), F32)
        for m in range(3):
            term = None
            for c in range(2):
                rows = g.buf[:, pl.ds(2 * pair, 2), c, m].reshape(4 * TOK, COL)
                one = mm(rows, g.turned[c, m])
                term = one if term is None else term + one
            here, there = term[:, :TOK], term[:, TOK:]
            acc = acc + here + mixes[:, m : m + 1] * (there - here)
        for i in range(4):
            to = 4 * i + pair
            g.y_out[to] = acc[i * TOK : (i + 1) * TOK].astype(BF16)

            @pl.when(to != h)
            def _():
                y_send(to).start()

    sums_first.wait_recv()
    acc = g.big_in[0]
    for n in range(1, N_SEQ):
        acc = acc + g.big_in[n]
    g.total[s] = acc[:16]
    sums_second = AllToAll("seq", N_SEQ, s, g.total, g.total, g.s_sems.at[6], g.s_sems.at[7], True)
    sums_second.start()
    g.base_grad[:, 0:128] = acc[16:17]
    g.base_grad[:, 128:256] = acc[17:18]
    g.bonus_grad[:, 0:128] = acc[18:19]
    g.bonus_grad[:, 128:256] = acc[19:20]

    edge_row.wait()
    gdi = g.gdi[...]
    next_row = jnp.where(s == N_SEQ - 1, 0.0, g.gdi_edge[0:1])
    later = jnp.where(tok == TOK - 1, next_row, pltpu.roll(gdi, TOK - 1, 0))
    mine = gdi + mix * (later - gdi)
    g.y_in[h] = g.y_out[h]
    loop(1, N_HEAD, lambda d: y_from((h + d) % N_HEAD).wait_recv())
    halves = []
    for c in range(2):
        acc = g.y_in[c].astype(F32)
        for y in range(1, 8):
            acc = acc + g.y_in[2 * y + c].astype(F32)
        halves.append(acc)
    lo, hi = halves
    joined = jnp.concatenate([lo[:64], hi[:64], lo[64:], hi[64:]], axis=0)
    g.out[...] = (joined.T + mine).astype(BF16)

    sums_second.wait_recv()
    g.down_grad[...] = g.total[0:16].reshape(COL, RANK)
    g.up_grad[:, 0:128] = g.total[16:24].reshape(RANK, 128)
    g.up_grad[:, 128:256] = g.total[24:32].reshape(RANK, 128)

    edge_copy.wait_send()
    for copies in (in_first, in_second, out_first, out_second, to_owner, to_range, sums_first, sums_second):
        copies.wait_send()
    loop(1, N_HEAD, lambda d: y_from((h + d) % N_HEAD).wait_send())
    weights.wait_send()


def step(*operands):
    return pl.pallas_call(
        step_kernel,
        out_shape=tuple(jax.ShapeDtypeStruct(*spec) for spec in OUTPUTS.values()),
        in_specs=[VMEM] * len(INPUTS),
        out_specs=(VMEM,) * len(OUTPUTS),
        scratch_shapes=list(SCRATCH.values()),
        compiler_params=pltpu.CompilerParams(
            collective_id=0, has_side_effects=True, vmem_limit_bytes=60 * 2**20
        ),
        name="step",
    )(*operands)


def per_device(
    layer_input, receptance, key_act, value_act, attention_result_sensitivity, time_first,
    decay_exponent_base, decay_shift_mix, mix_rkv, decay_adapter_down, decay_adapter_up, proj_weights,
):
    core = lax.axis_index("head") % 2
    mixes = lax.dynamic_index_in_dim(mix_rkv.reshape(3, 4, 4, 2, 2, 64), core, 4, keepdims=False)
    mixes = jnp.moveaxis(mixes, 2, 0).reshape(4, 3, 512)
    mixes = jnp.pad(mixes, ((0, 0), (0, 5), (0, 0)))
    out, down_grad, up_grad, base_grad, bonus_grad = step(
        layer_input, decay_shift_mix[None], decay_adapter_down, decay_exponent_base[None], decay_adapter_up,
        receptance, key_act, value_act, attention_result_sensitivity, time_first.reshape(1, COL),
        proj_weights, mixes,
    )
    return out, down_grad, up_grad, base_grad.reshape(COL), bonus_grad.reshape(4, HS)


def solution(mesh):
    return jax.shard_map(
        per_device,
        mesh=mesh,
        in_specs=(
            P("seq", "head"), P("seq", "head"), P("seq", "head"), P("seq", "head"), P("seq", "head"),
            P("head", None), P("head"), P("head"), P(), P("head", None), P(None, "head"),
            P(None, "seq", "head"),
        ),
        out_specs=(P("seq", "head"), P("head", None), P(None, "head"), P("head"), P("head", None)),
        check_vma=False,
    )
```

```python
from types import SimpleNamespace

import jax
import jax.numpy as jnp
from jax import lax
from jax.experimental import pallas as pl
from jax.experimental.pallas import tpu as pltpu
from jax.sharding import PartitionSpec as P

F32 = jnp.float32
BF16 = jnp.bfloat16
MESH = pl.DeviceIdType.MESH
N_HEAD = 16
N_SEQ = 32
TOK = 128
COL = 256
HS = 64
RANK = 128
VMEM = pl.BlockSpec(memory_space=pltpu.VMEM)

ROWS_LANES = (((1,), (0,)), ((), ()))
LANES_LANES = (((1,), (1,)), ((), ()))


def mm(a, b, dims=ROWS_LANES):
    return lax.dot_general(a, b, dims, preferred_element_type=F32)


def parts(a, count):
    out = []
    for _ in range(count - 1):
        top = a.astype(BF16)
        out.append(top)
        a = a - top.astype(F32)
    out.append(a.astype(BF16))
    return out


def mm3(a, b, dims=ROWS_LANES):
    ah, al = parts(a, 2)
    bh, bl = parts(b, 2)
    return mm(ah, bh, dims) + (mm(ah, bl, dims) + mm(al, bh, dims))


def mm_right_exact(a, b, dims=ROWS_LANES, count=2):
    out = None
    for piece in parts(a, count):
        term = mm(piece, b, dims)
        out = term if out is None else out + term
    return out


def mm_left_exact(a, b, dims=ROWS_LANES, count=2):
    out = None
    for piece in parts(b, count):
        term = mm(a, piece, dims)
        out = term if out is None else out + term
    return out


def iota(shape, dim):
    return lax.broadcasted_iota(jnp.int32, shape, dim)


def head_of(index):
    return index // HS


def lower_ones(strict):
    row, col = iota((TOK, TOK), 0), iota((TOK, TOK), 1)
    keep = row > col if strict else row >= col
    return jnp.where(keep, 1.0, 0.0).astype(BF16)


def upper_ones():
    row, col = iota((TOK, TOK), 0), iota((TOK, TOK), 1)
    return jnp.where(row < col, 1.0, 0.0).astype(BF16)


def block_diagonal():
    return head_of(iota((COL, COL), 0)) == head_of(iota((COL, COL), 1))


def odd_rows():
    return (head_of(iota((COL, 128), 0)) % 2) == 1


def remote(src, dst, send_sem, recv_sem, to):
    return pltpu.make_async_remote_copy(
        src_ref=src, dst_ref=dst, send_sem=send_sem, recv_sem=recv_sem,
        device_id=to, device_id_type=MESH,
    )


def greet(barrier, to):
    pl.semaphore_signal(barrier, inc=1, device_id=to, device_id_type=MESH)


def loop(start, stop, body):
    def step(i, carry):
        body(i)
        return carry

    lax.fori_loop(start, stop, step, 0)


def shift_mix(x, carried, mix):
    previous = pltpu.roll(x, 1, 0)
    previous = jnp.where(iota((TOK, COL), 0) == 0, carried, previous)
    return x + mix * (previous - x)


class AllToAll:
    def __init__(self, axis, size, me, out, land, sems, number, broadcast=False):
        self.axis, self.size, self.me = axis, size, me
        self.out, self.land, self.broadcast = out, land, broadcast
        self.send, self.recv = sems.at[number, 0], sems.at[number, 1]

    def start_one(self, peer):
        src = self.out.at[self.me if self.broadcast else peer]
        remote(src, self.land.at[self.me], self.send, self.recv, {self.axis: peer}).start()

    def start(self):
        loop(1, self.size, lambda d: self.start_one((self.me + d) % self.size))

    def _all(self):
        others = self.land.at[pl.ds(0, self.size - 1)]
        return remote(others, others, self.send, self.recv, {self.axis: (self.me + 1) % self.size})

    def wait_recv(self):
        self._all().wait_recv()

    def wait_send(self):
        self._all().wait_send()


class WeightGather:
    def __init__(self, g, h, s):
        self.g = g
        self.core = h % 2
        self.mate = h + 1 - 2 * self.core
        self.pair = h - self.core
        self.x, self.z = s // 8, s % 8

    def seq(self, x, z):
        return x * 8 + z

    def zz(self, d):
        return (self.z + d + 8) % 8

    def xx(self, d):
        return (self.x + d + 4) % 4

    def half(self, c):
        return self.g.w.at[:, pl.ds(pl.multiple_of(c * 64, 64), 64)]

    def land(self, x, z, src, kind):
        return self.g.buf.at[x, z, src], self.g.wrecv.at[kind, z]

    def arrived(self, blocks, z, kind):
        send = self.g.mate_send
        remote(blocks, blocks, send, self.g.wrecv.at[kind, z], {"head": self.mate}).wait_recv()

    def forward(self, x, z, src, way, kind, group):
        slot, sem = self.land(x, z, src, kind)
        place = (
            self.seq(self.x, self.zz(1)), self.seq(self.x, self.zz(-1)),
            self.seq(self.xx(1), self.z), self.seq(self.xx(-1), self.z),
        )[way]
        remote(slot, slot, self.g.wsend.at[group], sem, {"seq": place}).start()

    def sources(self, act):
        g, core = self.g, self.core
        dst = g.buf.at[self.x, self.z, core]
        act(remote(self.half(1 - core), dst, g.mate_send, g.mate_recv, {"head": self.mate}))

        @pl.when(core == 0)
        def _():
            dst, sem = self.land(self.x, self.z, 0, 0)
            for d in (1, 3, 2):
                place = self.seq(self.xx(d), self.z)
                for c in range(2):
                    act(remote(self.half(c), dst, g.first_send.at[d, c], sem, {"seq": place, "head": self.pair + c}))

        @pl.when(core == 1)
        def _():
            dst, sem = self.land(self.x, self.z, 1, 1)
            for d in (1, 3):
                place = self.seq(self.x, self.zz(1 if d == 1 else -1))
                for c in range(2):
                    act(remote(self.half(c), dst, g.first_send.at[d, c], sem, {"seq": place, "head": self.pair + c}))

    def keep_own(self):
        self.g.buf[self.x, self.z, self.core] = self.g.w[:, pl.ds(pl.multiple_of(self.core * 64, 64), 64)]

    def round_z0(self, d):
        for i in range(4 if d < 3 else 2):
            self.forward(i, self.zz(-d), 0, 0, 0, 0 if d < 3 else 2)
            self.forward(i if d < 3 else i + 2, self.zz(d), 0, 1, 0, 0 if d < 3 else 2)

    def round_z1(self, d):
        self.forward(self.x, self.zz(-d), 1, 0, 1, 2 if d < 3 else 3)
        if d < 3:
            self.forward(self.x, self.zz(d), 1, 1, 1, 2)

    def round_x1(self, d):
        z = self.zz(d)
        self.forward(self.x, z, 1, 2, 2, 1)
        self.forward(self.x, z, 1, 3, 2, 1)

    def turn_x1(self, d):
        z = self.zz(d)
        even = z % 2 == 0

        @pl.when(even)
        def _():
            self.forward(self.xx(-1), z, 1, 2, 3, 0)

        @pl.when(jnp.logical_not(even))
        def _():
            self.forward(self.xx(1), z, 1, 3, 3, 0)

    def wait_z0(self, d):
        z = self.zz(d)
        self.arrived(self.g.buf.at[:, z, 0], z, 0)

    def wait_own(self, d):
        z = self.zz(d)
        self.arrived(self.g.buf.at[self.x, z, 1], z, 1)

    def wait_sides(self, d):
        z = self.zz(d)
        self.arrived(self.g.buf.at[pl.ds(0, 2), z, 1], z, 2)

    def stage(self, number):
        g = self.g
        if number == 0:
            self.sources(lambda copy: copy.start())
        if number == 1:
            self.arrived(g.buf.at[pl.ds(0, 3), self.z, 0], self.z, 0)
            slot = g.buf.at[self.x, self.z, 1 - self.core]
            remote(slot, slot, g.mate_send, g.mate_recv, {"head": self.mate}).wait_recv()
            self.round_z0(0)
            self.round_x1(0)
            for d in (-1, 1):
                self.wait_own(d)
            self.round_z1(1)
            for d in (-1, 1):
                self.round_x1(d)
        if number == 2:
            for d in (-1, 1):
                self.wait_z0(d)
            self.round_z0(1)
            for d in (-2, 2):
                self.wait_own(d)
            self.round_z1(2)
            for d in (0, -1, 1):
                self.wait_sides(d)
                self.turn_x1(d)
            for d in (-2, 2):
                self.round_x1(d)
        if number == 3:
            for d in (-2, 2):
                self.wait_z0(d)
            self.round_z0(2)
            for d in (-3, 3):
                self.wait_own(d)
            self.round_z1(3)
            for d in (-2, 2):
                self.wait_sides(d)
                self.turn_x1(d)
            for d in (-3, 3):
                self.round_x1(d)
        if number == 4:
            for d in (-3, 3):
                self.wait_z0(d)
            self.round_z0(3)
            self.wait_own(4)
            self.round_x1(4)
            for d in (-3, 3):
                self.wait_sides(d)
                self.turn_x1(d)
        if number == 5:
            self.wait_z0(4)
            self.wait_sides(4)
            self.turn_x1(4)

    def far_side(self, z):
        self.arrived(self.g.buf.at[self.xx(2), z, 1], z, 3)

    def wait_send(self):
        g = self.g
        self.sources(lambda copy: copy.wait_send())
        waited = (g.buf.at[pl.ds(0, 2)], g.buf.at[0], g.buf.at[0, pl.ds(0, 4)], g.buf.at[0, 0, 0])
        for group, blocks in enumerate(waited):
            remote(blocks, blocks, g.wsend.at[group], g.mate_recv, {"head": self.mate}).wait_send()


INPUTS = {
    "x": ((TOK, COL), BF16),
    "mix": ((1, COL), F32),
    "down": ((COL, RANK), F32),
    "dy": ((TOK, COL), BF16),
    "v": ((TOK, COL), BF16),
    "w": ((3, TOK, COL), BF16),
    "base": ((1, COL), F32),
    "up": ((RANK, COL), F32),
    "r": ((TOK, COL), BF16),
    "k": ((TOK, COL), BF16),
    "u": ((4, HS), F32),
    "mixes": ((3, 4096), F32),
}
OUTPUTS = {
    "out": ((TOK, COL), BF16),
    "down_grad": ((COL, RANK), F32),
    "up_grad": ((RANK, COL), F32),
    "base_grad": ((1, COL), F32),
    "bonus_grad": ((8, HS), F32),
}
DMA = pltpu.SemaphoreType.DMA
SCRATCH = {
    **{name: pltpu.VMEM(*spec) for name, spec in INPUTS.items()},
    "in_sems": DMA((len(INPUTS),)),
    "mix_columns": pltpu.VMEM((4, 4 * TOK, 3), F32),
    "part1": pltpu.VMEM((N_HEAD, 8, 128), F32),
    "land1": pltpu.VMEM((N_HEAD, 8, 128), F32),
    "full1": pltpu.VMEM((N_HEAD, 8, 128), F32),
    "part2": pltpu.VMEM((N_HEAD, 8, 128), F32),
    "land2": pltpu.VMEM((N_HEAD, 8, 128), F32),
    "full2": pltpu.VMEM((N_HEAD, 8, 128), F32),
    "edge_part": pltpu.VMEM((8, 128), F32),
    "edge_land": pltpu.VMEM((N_HEAD, 8, 128), F32),
    "tail": pltpu.VMEM((16, COL), BF16),
    "pack": pltpu.VMEM((N_SEQ, 2, 8, 128), F32),
    "pack_in": pltpu.VMEM((N_SEQ, 2, 8, 128), F32),
    "back": pltpu.VMEM((N_SEQ, 8, 128), F32),
    "got": pltpu.VMEM((N_SEQ, 8, 128), F32),
    "pairs": pltpu.VMEM((8, TOK, COL), F32),
    "cross": pltpu.VMEM((4, TOK, 4 * TOK), BF16),
    "hold": pltpu.VMEM((8, TOK, COL), F32),
    "proj": pltpu.VMEM((2, 3, TOK, COL), BF16),
    "proj_edge": pltpu.VMEM((2, 3, 16, COL), BF16),
    "turned": pltpu.VMEM((2, 3, COL, 2 * TOK), BF16),
    "rise": pltpu.VMEM((N_SEQ, 16, 128), F32),
    "rise_in": pltpu.VMEM((N_SEQ, 16, 128), F32),
    "rise_total": pltpu.VMEM((N_SEQ, 8, 128), F32),
    "fall": pltpu.VMEM((N_SEQ, 8, 128), F32),
    "fall_in": pltpu.VMEM((N_SEQ, 8, 128), F32),
    "fall_total": pltpu.VMEM((N_SEQ, 8, 128), F32),
    "gdi": pltpu.VMEM((TOK, COL), F32),
    "gdi_edge": pltpu.VMEM((8, COL), F32),
    "y_out": pltpu.VMEM((N_HEAD, 128, TOK), BF16),
    "y_in": pltpu.VMEM((N_HEAD, 128, TOK), BF16),
    "buf": pltpu.VMEM((4, 8, 2, 3, 64, COL), BF16),
    "pair_sems": DMA((11, 2)),
    "one": DMA((12,)),
    "wrecv": DMA((4, 8)),
    "mate_recv": DMA,
    "wsend": DMA((4,)),
    "first_send": DMA((4, 2)),
    "mate_send": DMA,
}


def step_kernel(*refs):
    given, refs = refs[: len(INPUTS)], refs[len(INPUTS) :]
    g = SimpleNamespace(**dict(zip((*OUTPUTS, *SCRATCH), refs, strict=True)))
    fetches = {
        name: pltpu.make_async_copy(ref, getattr(g, name), g.in_sems.at[i])
        for i, (name, ref) in enumerate(zip(INPUTS, given, strict=True))
    }
    for fetch in fetches.values():
        fetch.start()
    h, s = lax.axis_index("head"), lax.axis_index("seq")
    core = h % 2
    mate = h + 1 - 2 * core
    nxt, prv = (s + 1) % N_SEQ, (s + N_SEQ - 1) % N_SEQ
    weights = WeightGather(g, h, s)

    barrier = pltpu.get_barrier_semaphore()
    loop(1, N_HEAD, lambda d: greet(barrier, {"head": (h + d) % N_HEAD}))

    def greet_seq(d):
        greet(barrier, {"seq": (s + d) % N_SEQ})
        greet(barrier, {"seq": (s + d) % N_SEQ, "head": mate})

    loop(1, N_SEQ, greet_seq)

    @pl.when(h == 0)
    def _():
        loop(0, N_HEAD, lambda j: greet(barrier, {"seq": prv, "head": j}))

    def fetched(*names):
        for name in names:
            fetches[name].wait()

    fetched("x", "mix", "down")
    x = g.x[...].astype(F32)
    mix = g.mix[...]
    down_h, down_l = parts(g.down[...], 2)

    def into_rank(a):
        a_h, a_l = parts(a, 2)
        return mm(a_h, down_h) + (mm(a_h, down_l) + mm(a_l, down_h))

    g.part1[...] = into_rank(shift_mix(x, 0.0, mix)).reshape(N_HEAD, 8, 128)
    g.edge_part[...] = into_rank(mix * x[TOK - 8 :])
    g.land1[h] = g.part1[h]
    fetched("w")
    weights.keep_own()
    fetched("dy", "v", "r", "k", "u", "base", "up", "mixes")
    pl.semaphore_wait(barrier, N_HEAD - 1 + 2 * (N_SEQ - 1) + 1)
    in_first = AllToAll("head", N_HEAD, h, g.part1, g.land1, g.pair_sems, 0)
    in_first.start()
    edge_copy = remote(g.edge_part, g.edge_land.at[h], g.one.at[2], g.one.at[11], {"seq": nxt, "head": 0})
    edge_copy.start()
    weights.stage(0)
    row_copy = remote(g.x.at[pl.ds(TOK - 16, 16)], g.tail, g.one.at[0], g.one.at[1], {"seq": nxt})
    row_copy.start()

    rb, kb, vb, dyb = g.r[...], g.k[...], g.v[...], g.dy[...]
    r, k, v, dy = (a.astype(F32) for a in (rb, kb, vb, dyb))
    own = block_diagonal()
    odd = odd_rows()
    lane_head = head_of(iota((TOK, COL), 1))
    heads = [lane_head == i for i in range(4)]
    zero16 = jnp.zeros((TOK, COL), BF16)

    def by_head(a):
        return jnp.concatenate([jnp.where(m, a, zero16) for m in heads], axis=0)

    def lane_cat(stacked):
        return jnp.concatenate([stacked[i * TOK : (i + 1) * TOK] for i in range(4)], axis=1)

    spread = jnp.where(own, 1.0, 0.0).astype(BF16)
    unfold = jnp.where(iota((HS, COL), 0) == iota((HS, COL), 1) % HS, 1.0, 0.0).astype(BF16)
    head_rows = iota((8, COL), 0) == head_of(iota((8, COL), 1))
    u = jnp.concatenate([g.u[...], jnp.zeros((4, HS), F32)], axis=0)
    u = jnp.sum(jnp.where(head_rows, mm_right_exact(u, unfold, count=3), 0.0), axis=0, keepdims=True)

    def tiles(a):
        return a.reshape(TOK // 8, 8, COL)

    def flat(a):
        return a.reshape(TOK, COL)

    for i, piece in enumerate(parts(mm(by_head(dyb), vb, LANES_LANES), 2)):
        g.cross[i] = lane_cat(piece)
    for i, piece in enumerate(parts(mm(by_head(vb), dyb, LANES_LANES), 2)):
        g.cross[2 + i] = lane_cat(piece)
    for d in range(8):
        v_old = v if d == 0 else flat(pltpu.roll(tiles(v), d, 1))
        g.pairs[d] = mm_right_exact(dy * v_old, spread)

    in_first.wait_recv()

    @pl.when(h == 0)
    def _():
        remote(g.edge_land, g.edge_land, g.one.at[2], g.one.at[11], {"seq": nxt}).wait_recv()
        rows = g.edge_land[0]
        for j in range(1, N_HEAD):
            rows = rows + g.edge_land[j]
        first_row = jnp.where((iota((8, 128), 0) == 0) & (s > 0), pltpu.roll(rows, 1, 0), 0.0)
        g.land1[0] = g.land1[0] + first_row

    def summed(ref):
        acc = ref[0]
        for j in range(1, N_HEAD):
            acc = acc + ref[j]
        return acc

    g.full1[h] = summed(g.land1)
    in_second = AllToAll("head", N_HEAD, h, g.full1, g.full1, g.pair_sems, 1, True)
    in_second.start()
    weights.stage(1)
    in_second.wait_recv()

    mid = jnp.tanh(g.full1[...].reshape(TOK, RANK))
    up_h, up_l = parts(g.up[...], 2)
    mid_h, mid_l = parts(mid, 2)
    w = -jnp.exp(g.base[...] + (mm(mid_h, up_h) + (mm(mid_h, up_l) + mm(mid_l, up_h))))
    w_parts = parts(w, 3)
    ones = lower_ones(False)
    cumul = mm(ones, w_parts[0]) + (mm(ones, w_parts[1]) + mm(ones, w_parts[2]))
    before = cumul - w
    final = cumul[TOK - 1 : TOK]
    all_ones = jnp.ones((TOK, 128), BF16)
    w_turned = [p.astype(F32).T.astype(BF16) for p in w_parts]
    total_rows = mm(w_turned[0], all_ones) + (mm(w_turned[1], all_ones) + mm(w_turned[2], all_ones))
    to_end = jnp.exp(jnp.minimum(final - cumul, 0.0))
    from_start = jnp.exp(before)

    def folded(a, b):
        wide = jnp.where(own, mm_right_exact(a.T, b), 0.0)
        return wide[:, :128] + wide[:, 128:]

    state = folded(k * to_end, vb)
    grad = folded(r * from_start, dyb)
    packed = jnp.where(odd, pltpu.roll(state, 64, 1), state) + jnp.where(odd, grad, pltpu.roll(grad, 64, 1))
    g.pack[:, 0] = packed.reshape(N_SEQ, 8, 128)
    g.pack[:, 1] = jnp.exp(total_rows).reshape(N_SEQ, 8, 128)
    to_owner = AllToAll("seq", N_SEQ, s, g.pack, g.pack_in, g.pair_sems, 4)
    to_owner.start()
    g.pack_in[s] = g.pack[s]
    g.hold[0], g.hold[1], g.hold[2], g.hold[3] = w, cumul, to_end, from_start

    gr_mem = jnp.zeros((TOK, COL), F32)
    gk_in = jnp.zeros((TOK, COL), F32)
    score_st = jnp.zeros((4 * TOK, TOK), F32)
    tok = iota((TOK, COL), 0)

    def wide_mm(first, mask, factor):
        f_top, f_low = (by_head(p) for p in parts(factor, 2))
        zero = jnp.zeros((TOK, 4 * TOK), BF16)
        top, low = jnp.where(mask, g.cross[first], zero), jnp.where(mask, g.cross[first + 1], zero)
        return mm(top, f_top) + (mm(top, f_low) + mm(low, f_top))

    for half in (64, 32, 16, 8):
        size = 2 * half
        second = (tok % size) >= half
        middle = cumul.reshape(TOK // size, size, COL)[:, half - 1 : half]
        middle = jnp.broadcast_to(middle, (TOK // size, size, COL)).reshape(TOK, COL)
        fade = jnp.exp(jnp.minimum(jnp.where(second, before - middle, middle - cumul), 0.0))
        late, early = jnp.where(second, fade, 0.0), jnp.where(second, 0.0, fade)
        r_hat, k_hat = r * late, k * early
        same = iota((TOK, 4 * TOK), 0) // size == (iota((TOK, 4 * TOK), 1) % TOK) // size
        gr_mem = gr_mem + late * wide_mm(0, same, k_hat)
        gk_in = gk_in + early * wide_mm(2, same, r_hat)
        k_top, k_low = (by_head(p) for p in parts(k_hat, 2))
        r_top, r_low = parts(r_hat, 2)
        score = mm(k_top, r_top, LANES_LANES) + (mm(k_top, r_low, LANES_LANES) + mm(k_low, r_top, LANES_LANES))
        same_st = (iota((4 * TOK, TOK), 0) % TOK) // size == iota((4 * TOK, TOK), 1) // size
        score_st = score_st + jnp.where(same_st, score, 0.0)
    gv = jnp.zeros((TOK, COL), F32)
    dy_heads = by_head(dyb)
    for piece in parts(score_st, 2):
        gv = gv + mm(lane_cat(piece), dy_heads)

    weights.stage(2)
    to_owner.wait_recv()
    onward = jnp.zeros((8, 128), F32)
    forward = []
    for n in range(N_SEQ):
        forward.append(onward)
        onward = g.pack_in[n, 1] * onward + g.pack_in[n, 0]
    left8 = iota((8, 128), 1) < 64
    reverse = jnp.zeros((8, 128), F32)
    for n in reversed(range(N_SEQ)):
        g.back[n] = jnp.where(left8, forward[n], reverse)
        reverse = g.pack_in[n, 1] * reverse + g.pack_in[n, 0]
    to_range = AllToAll("seq", N_SEQ, s, g.back, g.got, g.pair_sems, 5)
    to_range.start()
    g.got[s] = g.back[s]

    sub = iota((TOK // 8, 8, COL), 1)
    for d in range(1, 8):
        valid = sub >= d
        cum_old = pltpu.roll(tiles(cumul), d, 1)
        k_old = flat(pltpu.roll(tiles(k), d, 1))
        fade = jnp.exp(jnp.minimum(jnp.where(valid, tiles(before) - cum_old, 0.0), 0.0))
        fade = flat(jnp.where(valid, fade, 0.0))
        pair = g.pairs[d]
        faded_r = fade * r
        gr_mem = gr_mem + fade * pair * k_old
        gk_in = gk_in + flat(pltpu.roll(tiles(faded_r * pair), 8 - d, 1))
        score = mm_right_exact(faded_r * k_old, spread)
        gv = gv + flat(pltpu.roll(tiles(score * dy), 8 - d, 1))
    gv = gv + mm_right_exact(r * u * k, spread) * dy
    g.hold[4], g.hold[5], g.hold[6] = gr_mem, gk_in, gv
    weights.stage(3)
    to_range.wait_recv()

    w, cumul, to_end, from_start = g.hold[0], g.hold[1], g.hold[2], g.hold[3]
    packed = g.got[...].reshape(COL, 128)
    left = iota((COL, 128), 1) < 64
    state, grad = jnp.where(left, packed, 0.0), jnp.where(left, 0.0, packed)
    state = jnp.where(odd, pltpu.roll(state, 64, 1), state)
    grad = jnp.where(odd, grad, pltpu.roll(grad, 64, 1))
    state = jnp.where(own, jnp.concatenate([state, state], axis=1), 0.0)
    grad = jnp.where(own, jnp.concatenate([grad, grad], axis=1), 0.0)
    gr_mem = g.hold[4] + from_start * mm_left_exact(dyb, state, LANES_LANES)
    gk_in = g.hold[5]
    gk_out = to_end * mm_left_exact(vb, grad, LANES_LANES)
    across = mm_left_exact(jnp.ones((8, COL), BF16), state * grad, LANES_LANES, 3)[0:1]
    across = across * jnp.exp(cumul[TOK - 1 : TOK])
    k_in = k * gk_in
    g_log = across - k_in + mm_left_exact(lower_ones(True), k * gk_out)
    g_log = g_log + mm_left_exact(upper_ones(), r * gr_mem - k_in)
    g_pre = g_log * w
    g.part2[...] = mm3(g_pre, g.up[...], LANES_LANES).reshape(N_HEAD, 8, 128)
    out_first = AllToAll("head", N_HEAD, h, g.part2, g.land2, g.pair_sems, 2)
    out_first.start()
    g.land2[h] = g.part2[h]

    self_pair = g.pairs[0]
    r_pair = r * self_pair
    g.proj[core, 0] = (gr_mem + u * k * self_pair).astype(BF16)
    g.proj[core, 1] = (gk_in + gk_out + u * r_pair).astype(BF16)
    g.proj[core, 2] = (g.hold[6] + mm3(k * to_end, grad)).astype(BF16)
    swap = remote(g.proj.at[core], g.proj.at[core], g.one.at[3], g.one.at[4], {"head": mate})
    first_rows = g.proj.at[core, :, pl.ds(0, 16)]
    near = remote(first_rows, g.proj_edge.at[core], g.one.at[5], g.one.at[6], {"seq": prv})
    far = remote(first_rows, g.proj_edge.at[core], g.one.at[7], g.one.at[8], {"seq": prv, "head": mate})
    swap.start()
    near.start()
    far.start()
    raising = mm3(mid.T, g_pre)
    g.rise[0:16, 0:8] = raising[:, 0:128].reshape(16, 8, 128)
    g.rise[16:32, 0:8] = raising[:, 128:256].reshape(16, 8, 128)
    floor_row = jnp.sum(g_pre, axis=0, keepdims=True)
    bonus_row = jnp.sum(k * r_pair, axis=0, keepdims=True)
    row8 = iota((8, 128), 0)
    small = jnp.where(row8 == 0, floor_row[:, :128], 0.0) + jnp.where(row8 == 1, floor_row[:, 128:], 0.0)
    small = small + jnp.where(row8 == 2, bonus_row[:, :128], 0.0) + jnp.where(row8 == 3, bonus_row[:, 128:], 0.0)
    g.rise[:, 8:16] = jnp.broadcast_to(small[None], (N_SEQ, 8, 128))
    rise_first = AllToAll("seq", N_SEQ, s, g.rise, g.rise_in, g.pair_sems, 6)
    rise_first.start()
    g.rise_in[s] = g.rise[s]
    row_copy.wait()
    carried = jnp.where(s == 0, 0.0, g.tail[...].astype(F32)[15:16])
    turned_in = shift_mix(x, carried, mix).T

    out_first.wait_recv()
    g.full2[h] = summed(g.land2)
    out_second = AllToAll("head", N_HEAD, h, g.full2, g.full2, g.pair_sems, 3, True)
    out_second.start()
    weights.stage(4)

    swap.wait()
    near.wait()
    far.wait()
    for c in range(2):
        for m in range(3):
            a = g.proj[c, m].astype(F32)
            edge = jnp.where(s == N_SEQ - 1, 0.0, g.proj_edge[c, m].astype(F32)[0:1])
            later = jnp.where(tok == TOK - 1, edge, pltpu.roll(a, TOK - 1, 0))
            g.turned[c, m, :, 0:TOK] = a.T.astype(BF16)
            g.turned[c, m, :, TOK:] = later.T.astype(BF16)
    for pair in range(4):
        columns = []
        for i in range(4):
            for p in range(2):
                place = 8 * i + 2 * pair + p
                column = g.mixes[:, place * 128 : (place + 1) * 128].T
                columns.append(jnp.where(core == 0, column[:64], column[64:]))
        g.mix_columns[pair] = jnp.concatenate(columns, axis=0)
    out_second.wait_recv()

    g_mid = g.full2[...].reshape(TOK, RANK) * (1.0 - mid * mid)
    g.fall[...] = mm3(turned_in, g_mid).reshape(N_SEQ, 8, 128)
    fall_first = AllToAll("seq", N_SEQ, s, g.fall, g.fall_in, g.pair_sems, 7)
    fall_first.start()
    gdi = mm3(g_mid, g.down[...], LANES_LANES)
    g.gdi[...] = gdi
    edge_row = remote(g.gdi.at[pl.ds(0, 8)], g.gdi_edge, g.one.at[9], g.one.at[10], {"seq": prv})
    edge_row.start()
    g.fall_in[s] = g.fall[s]

    def summed_seq(ref):
        acc = ref[0]
        for n in range(1, N_SEQ):
            acc = acc + ref[n]
        return acc

    y_copy = AllToAll("head", N_HEAD, h, g.y_out, g.y_in, g.pair_sems, 10)
    near_pair = (s % 8) // 2
    for turn in (0, 1, 3, 2):
        pair = (near_pair + turn) % 4
        if turn == 2:
            weights.stage(5)
        weights.far_side(2 * pair)
        weights.far_side(2 * pair + 1)
        mixes = g.mix_columns[pair]
        acc = jnp.zeros((4 * TOK, TOK), F32)
        for m in range(3):
            term = None
            for c in range(2):
                rows = g.buf[:, pl.ds(2 * pair, 2), c, m].reshape(4 * TOK, COL)
                one = mm(rows, g.turned[c, m])
                term = one if term is None else term + one
            here, there = term[:, :TOK], term[:, TOK:]
            acc = acc + here + mixes[:, m : m + 1] * (there - here)
        for i in range(4):
            to = 4 * i + pair
            g.y_out[to] = acc[i * TOK : (i + 1) * TOK].astype(BF16)

            @pl.when(to != h)
            def _():
                y_copy.start_one(to)

        if turn == 0:
            rise_first.wait_recv()
            acc = summed_seq(g.rise_in)
            g.rise_total[s] = acc[:8]
            rise_second = AllToAll("seq", N_SEQ, s, g.rise_total, g.rise_total, g.pair_sems, 8, True)
            rise_second.start()
            g.base_grad[:, 0:128] = acc[8:9]
            g.base_grad[:, 128:256] = acc[9:10]
            bonus = jnp.concatenate([acc[10:11], acc[11:12]], axis=1)
            bonus = jnp.where(head_rows, bonus, 0.0)
            rows = None
            for piece in parts(bonus, 3):
                one = mm(piece, unfold, LANES_LANES)
                rows = one if rows is None else rows + one
            g.bonus_grad[...] = rows
    fall_first.wait_recv()
    g.fall_total[s] = summed_seq(g.fall_in)
    fall_second = AllToAll("seq", N_SEQ, s, g.fall_total, g.fall_total, g.pair_sems, 9, True)
    fall_second.start()

    edge_row.wait()
    gdi = g.gdi[...]
    next_row = jnp.where(s == N_SEQ - 1, 0.0, g.gdi_edge[0:1])
    later = jnp.where(tok == TOK - 1, next_row, pltpu.roll(gdi, TOK - 1, 0))
    mine = gdi + mix * (later - gdi)
    g.y_in[h] = g.y_out[h]
    y_copy.wait_recv()
    halves = []
    for c in range(2):
        acc = g.y_in[c].astype(F32)
        for y in range(1, 8):
            acc = acc + g.y_in[2 * y + c].astype(F32)
        halves.append(acc)
    lo, hi = halves
    joined = jnp.concatenate([lo[:64], hi[:64], lo[64:], hi[64:]], axis=0)
    g.out[...] = (joined.T + mine).astype(BF16)

    edge_copy.wait_send()
    for copies in (
        in_first, in_second, out_first, out_second, to_owner, to_range, rise_first, rise_second, fall_first, y_copy,
    ):
        copies.wait_send()
    weights.wait_send()
    rise_second.wait_recv()
    g.up_grad[:, 0:128] = g.rise_total[0:16].reshape(RANK, 128)
    g.up_grad[:, 128:256] = g.rise_total[16:32].reshape(RANK, 128)
    fall_second.wait_recv()
    g.down_grad[...] = g.fall_total[...].reshape(COL, RANK)
    fall_second.wait_send()


def step(*operands):
    return pl.pallas_call(
        step_kernel,
        out_shape=tuple(jax.ShapeDtypeStruct(*spec) for spec in OUTPUTS.values()),
        in_specs=[pl.BlockSpec(memory_space=pl.ANY)] * len(INPUTS),
        out_specs=(VMEM,) * len(OUTPUTS),
        scratch_shapes=list(SCRATCH.values()),
        compiler_params=pltpu.CompilerParams(
            collective_id=0, has_side_effects=True, vmem_limit_bytes=60 * 2**20
        ),
        name="step",
    )(*operands)


def finish_kernel(out_in, down_in, up_in, base_in, bonus_in, out, down_grad, up_grad, base_grad, bonus_grad):
    out[...] = out_in[...]
    down_grad[...] = down_in[...]
    up_grad[...] = up_in[...]
    base_grad[...] = base_in[...].reshape(COL)
    bonus_grad[...] = bonus_in[0:4]


def finish(*results):
    return pl.pallas_call(
        finish_kernel,
        out_shape=(
            *(jax.ShapeDtypeStruct(*spec) for spec in list(OUTPUTS.values())[:3]),
            jax.ShapeDtypeStruct((COL,), F32),
            jax.ShapeDtypeStruct((4, HS), F32),
        ),
        in_specs=[VMEM] * 5,
        out_specs=(VMEM,) * 5,
        name="finish",
    )(*results)


def per_device(
    layer_input, receptance, key_act, value_act, attention_result_sensitivity, time_first,
    decay_exponent_base, decay_shift_mix, mix_rkv, decay_adapter_down, decay_adapter_up, proj_weights,
):
    given = {
        "x": layer_input, "mix": decay_shift_mix[None], "down": decay_adapter_down,
        "base": decay_exponent_base[None], "up": decay_adapter_up, "r": receptance, "k": key_act,
        "v": value_act, "dy": attention_result_sensitivity, "u": time_first, "w": proj_weights, "mixes": mix_rkv,
    }
    return finish(*step(*(given[name] for name in INPUTS)))


def solution(mesh):
    return jax.shard_map(
        per_device,
        mesh=mesh,
        in_specs=(
            P("seq", "head"), P("seq", "head"), P("seq", "head"), P("seq", "head"), P("seq", "head"),
            P("head", None), P("head"), P("head"), P(), P("head", None), P(None, "head"),
            P(None, "seq", "head"),
        ),
        out_specs=(P("seq", "head"), P("head", None), P(None, "head"), P("head"), P("head", None)),
        check_vma=False,
    )
```

```python
from types import SimpleNamespace

import jax
import jax.numpy as jnp
from jax import lax
from jax.experimental import pallas as pl
from jax.experimental.pallas import tpu as pltpu
from jax.sharding import PartitionSpec as P

F32 = jnp.float32
BF16 = jnp.bfloat16
MESH = pl.DeviceIdType.MESH
N_HEAD = 16
N_SEQ = 32
TOK = 128
COL = 256
HS = 64
RANK = 128
VMEM = pl.BlockSpec(memory_space=pltpu.VMEM)

ROWS_LANES = (((1,), (0,)), ((), ()))
LANES_LANES = (((1,), (1,)), ((), ()))


def mm(a, b, dims=ROWS_LANES):
    return lax.dot_general(a, b, dims, preferred_element_type=F32)


def parts(a, count):
    out = []
    for _ in range(count - 1):
        top = a.astype(BF16)
        out.append(top)
        a = a - top.astype(F32)
    out.append(a.astype(BF16))
    return out


def mm3(a, b, dims=ROWS_LANES):
    ah, al = parts(a, 2)
    bh, bl = parts(b, 2)
    return mm(ah, bh, dims) + (mm(ah, bl, dims) + mm(al, bh, dims))


def mm_right_exact(a, b, dims=ROWS_LANES, count=2):
    out = None
    for piece in parts(a, count):
        term = mm(piece, b, dims)
        out = term if out is None else out + term
    return out


def mm_left_exact(a, b, dims=ROWS_LANES, count=2):
    out = None
    for piece in parts(b, count):
        term = mm(a, piece, dims)
        out = term if out is None else out + term
    return out


def iota(shape, dim):
    return lax.broadcasted_iota(jnp.int32, shape, dim)


def head_of(index):
    return index // HS


def lower_ones(strict):
    row, col = iota((TOK, TOK), 0), iota((TOK, TOK), 1)
    keep = row > col if strict else row >= col
    return jnp.where(keep, 1.0, 0.0).astype(BF16)


def upper_ones():
    row, col = iota((TOK, TOK), 0), iota((TOK, TOK), 1)
    return jnp.where(row < col, 1.0, 0.0).astype(BF16)


def block_diagonal():
    return head_of(iota((COL, COL), 0)) == head_of(iota((COL, COL), 1))


def odd_rows():
    return (head_of(iota((COL, 128), 0)) % 2) == 1


def remote(src, dst, send_sem, recv_sem, to):
    return pltpu.make_async_remote_copy(
        src_ref=src, dst_ref=dst, send_sem=send_sem, recv_sem=recv_sem,
        device_id=to, device_id_type=MESH,
    )


def greet(barrier, to):
    pl.semaphore_signal(barrier, inc=1, device_id=to, device_id_type=MESH)


def loop(start, stop, body):
    def step(i, carry):
        body(i)
        return carry

    lax.fori_loop(start, stop, step, 0)


def shift_mix(x, carried, mix):
    previous = pltpu.roll(x, 1, 0)
    previous = jnp.where(iota((TOK, COL), 0) == 0, carried, previous)
    return x + mix * (previous - x)


class AllToAll:
    def __init__(self, axis, size, me, out, land, sems, number, broadcast=False):
        self.axis, self.size, self.me = axis, size, me
        self.out, self.land, self.broadcast = out, land, broadcast
        self.send, self.recv = sems.at[number, 0], sems.at[number, 1]

    def start_one(self, peer):
        src = self.out.at[self.me if self.broadcast else peer]
        remote(src, self.land.at[self.me], self.send, self.recv, {self.axis: peer}).start()

    def start(self):
        loop(1, self.size, lambda d: self.start_one((self.me + d) % self.size))

    def _all(self):
        others = self.land.at[pl.ds(0, self.size - 1)]
        return remote(others, others, self.send, self.recv, {self.axis: (self.me + 1) % self.size})

    def wait_recv(self):
        self._all().wait_recv()

    def wait_send(self):
        self._all().wait_send()


class WeightGather:
    def __init__(self, g, h, s):
        self.g = g
        self.core = h % 2
        self.mate = h + 1 - 2 * self.core
        self.pair = h - self.core
        self.x, self.z = s // 8, s % 8

    def seq(self, x, z):
        return x * 8 + z

    def zz(self, d):
        return (self.z + d + 8) % 8

    def xx(self, d):
        return (self.x + d + 4) % 4

    def half(self, c):
        return self.g.w.at[:, pl.ds(pl.multiple_of(c * 64, 64), 64)]

    def land(self, x, z, src, kind):
        return self.g.buf.at[x, z, src], self.g.zrecv.at[x, z] if kind == 0 else self.g.wrecv.at[kind - 1, z]

    def arrived(self, blocks, z, kind):
        send = self.g.mate_send
        remote(blocks, blocks, send, self.g.wrecv.at[kind - 1, z], {"head": self.mate}).wait_recv()

    def forward(self, x, z, src, way, kind, group):
        slot, sem = self.land(x, z, src, kind)
        place = (
            self.seq(self.x, self.zz(1)), self.seq(self.x, self.zz(-1)),
            self.seq(self.xx(1), self.z), self.seq(self.xx(-1), self.z),
        )[way]
        remote(slot, slot, self.g.wsend.at[group], sem, {"seq": place}).start()

    def sources(self, act):
        g, core = self.g, self.core
        dst = g.buf.at[self.x, self.z, core]
        act(remote(self.half(1 - core), dst, g.mate_send, g.mate_recv, {"head": self.mate}))

        @pl.when(core == 0)
        def _():
            dst, sem = self.land(self.x, self.z, 0, 0)
            for d in (1, 3, 2):
                place = self.seq(self.xx(d), self.z)
                for c in range(2):
                    act(remote(self.half(c), dst, g.first_send.at[d, c], sem, {"seq": place, "head": self.pair + c}))

        @pl.when(core == 1)
        def _():
            dst, sem = self.land(self.x, self.z, 1, 1)
            for d in (1, 3):
                place = self.seq(self.x, self.zz(1 if d == 1 else -1))
                for c in range(2):
                    act(remote(self.half(c), dst, g.first_send.at[d, c], sem, {"seq": place, "head": self.pair + c}))

    def keep_own(self):
        self.g.buf[self.x, self.z, self.core] = self.g.w[:, pl.ds(pl.multiple_of(self.core * 64, 64), 64)]

    def wait_z0(self, j, d):
        slot, sem = self.land(self.xx(j), self.zz(d), 0, 0)
        remote(slot, slot, self.g.mate_send, sem, {"head": self.mate}).wait_recv()

    def round_z0(self, d):
        for j in (0, 1, 3, 2):
            up, down = d < 3 or j in (0, 1), d < 3 or j in (3, 2)
            if d == 0 and j != 0:
                self.wait_z0(j, 0)
            if d > 0:
                self.wait_z0(j, -d)
            if up:
                self.forward(self.xx(j), self.zz(-d), 0, 0, 0, 0 if d < 3 else 2)
            if d > 0:
                self.wait_z0(j, d)
            if down:
                self.forward(self.xx(j), self.zz(d), 0, 1, 0, 0 if d < 3 else 2)

    def round_z1(self, d):
        self.forward(self.x, self.zz(-d), 1, 0, 1, 2 if d < 3 else 3)
        if d < 3:
            self.forward(self.x, self.zz(d), 1, 1, 1, 2)

    def round_x1(self, d):
        z = self.zz(d)
        self.forward(self.x, z, 1, 2, 2, 1)
        self.forward(self.x, z, 1, 3, 2, 1)

    def turn_x1(self, d):
        z = self.zz(d)
        even = z % 2 == 0

        @pl.when(even)
        def _():
            self.forward(self.xx(-1), z, 1, 2, 3, 0)

        @pl.when(jnp.logical_not(even))
        def _():
            self.forward(self.xx(1), z, 1, 3, 3, 0)

    def wait_own(self, d):
        z = self.zz(d)
        self.arrived(self.g.buf.at[self.x, z, 1], z, 1)

    def wait_sides(self, d):
        z = self.zz(d)
        self.arrived(self.g.buf.at[pl.ds(0, 2), z, 1], z, 2)

    def stage(self, number):
        g = self.g
        if number == 0:
            self.sources(lambda copy: copy.start())
        if number == 1:
            slot = g.buf.at[self.x, self.z, 1 - self.core]
            remote(slot, slot, g.mate_send, g.mate_recv, {"head": self.mate}).wait_recv()
            self.round_x1(0)
            for d in (-1, 1):
                self.wait_own(d)
            self.round_z1(1)
            for d in (-1, 1):
                self.round_x1(d)
            self.round_z0(0)
        if number == 2:
            for d in (-2, 2):
                self.wait_own(d)
            self.round_z1(2)
            for d in (0, -1, 1):
                self.wait_sides(d)
                self.turn_x1(d)
            for d in (-2, 2):
                self.round_x1(d)
            self.round_z0(1)
        if number == 3:
            for d in (-3, 3):
                self.wait_own(d)
            self.round_z1(3)
            for d in (-2, 2):
                self.wait_sides(d)
                self.turn_x1(d)
            for d in (-3, 3):
                self.round_x1(d)
            self.round_z0(2)
        if number == 4:
            self.wait_own(4)
            self.round_x1(4)
            for d in (-3, 3):
                self.wait_sides(d)
                self.turn_x1(d)
            self.round_z0(3)
        if number == 5:
            self.wait_sides(4)
            self.turn_x1(4)
        if number == 6:
            for j in (0, 1, 3, 2):
                self.wait_z0(j, 4)

    def far_side(self, z):
        self.arrived(self.g.buf.at[self.xx(2), z, 1], z, 3)

    def wait_send(self):
        g = self.g
        self.sources(lambda copy: copy.wait_send())
        waited = (g.buf.at[pl.ds(0, 2)], g.buf.at[0], g.buf.at[0, pl.ds(0, 4)], g.buf.at[0, 0, 0])
        for group, blocks in enumerate(waited):
            remote(blocks, blocks, g.wsend.at[group], g.mate_recv, {"head": self.mate}).wait_send()


INPUTS = {
    "x": ((TOK, COL), BF16),
    "mix": ((1, COL), F32),
    "down": ((COL, RANK), F32),
    "dy": ((TOK, COL), BF16),
    "v": ((TOK, COL), BF16),
    "w": ((3, TOK, COL), BF16),
    "base": ((1, COL), F32),
    "up": ((RANK, COL), F32),
    "r": ((TOK, COL), BF16),
    "k": ((TOK, COL), BF16),
    "u": ((4, HS), F32),
    "mixes": ((3, 4096), F32),
}
OUTPUTS = {
    "out": ((TOK, COL), BF16),
    "down_grad": ((COL, RANK), F32),
    "up_grad": ((RANK, COL), F32),
    "base_grad": ((1, COL), F32),
    "bonus_grad": ((8, HS), F32),
}
DMA = pltpu.SemaphoreType.DMA
SCRATCH = {
    **{name: pltpu.VMEM(*spec) for name, spec in INPUTS.items()},
    "in_sems": DMA((len(INPUTS),)),
    "mix_columns": pltpu.VMEM((4, 4 * TOK, 3), F32),
    "part1": pltpu.VMEM((N_HEAD, 8, 128), F32),
    "land1": pltpu.VMEM((N_HEAD, 8, 128), F32),
    "full1": pltpu.VMEM((N_HEAD, 8, 128), F32),
    "part2": pltpu.VMEM((N_HEAD, 8, 128), F32),
    "land2": pltpu.VMEM((N_HEAD, 8, 128), F32),
    "full2": pltpu.VMEM((N_HEAD, 8, 128), F32),
    "edge_part": pltpu.VMEM((8, 128), F32),
    "edge_land": pltpu.VMEM((N_HEAD, 8, 128), F32),
    "tail": pltpu.VMEM((16, COL), BF16),
    "pack": pltpu.VMEM((N_SEQ, 2, 8, 128), F32),
    "pack_in": pltpu.VMEM((N_SEQ, 2, 8, 128), F32),
    "back": pltpu.VMEM((N_SEQ, 8, 128), F32),
    "got": pltpu.VMEM((N_SEQ, 8, 128), F32),
    "pairs": pltpu.VMEM((8, TOK, COL), F32),
    "cross": pltpu.VMEM((4, TOK, 4 * TOK), BF16),
    "hold": pltpu.VMEM((8, TOK, COL), F32),
    "proj": pltpu.VMEM((2, 3, TOK, COL), BF16),
    "proj_edge": pltpu.VMEM((2, 3, 16, COL), BF16),
    "turned": pltpu.VMEM((2, 3, COL, 2 * TOK), BF16),
    "rise": pltpu.VMEM((N_SEQ, 16, 128), F32),
    "rise_in": pltpu.VMEM((N_SEQ, 16, 128), F32),
    "rise_total": pltpu.VMEM((N_SEQ, 8, 128), F32),
    "fall": pltpu.VMEM((N_SEQ, 8, 128), F32),
    "fall_in": pltpu.VMEM((N_SEQ, 8, 128), F32),
    "fall_total": pltpu.VMEM((N_SEQ, 8, 128), F32),
    "gdi": pltpu.VMEM((TOK, COL), F32),
    "gdi_edge": pltpu.VMEM((8, COL), F32),
    "y_out": pltpu.VMEM((N_HEAD, 128, TOK), BF16),
    "y_in": pltpu.VMEM((N_HEAD, 128, TOK), BF16),
    "buf": pltpu.VMEM((4, 8, 2, 3, 64, COL), BF16),
    "pair_sems": DMA((11, 2)),
    "one": DMA((12,)),
    "zrecv": DMA((4, 8)),
    "wrecv": DMA((3, 8)),
    "mate_recv": DMA,
    "wsend": DMA((4,)),
    "first_send": DMA((4, 2)),
    "mate_send": DMA,
}


def step_kernel(*refs):
    given, refs = refs[: len(INPUTS)], refs[len(INPUTS) :]
    g = SimpleNamespace(**dict(zip((*OUTPUTS, *SCRATCH), refs, strict=True)))
    fetches = {
        name: pltpu.make_async_copy(ref, getattr(g, name), g.in_sems.at[i])
        for i, (name, ref) in enumerate(zip(INPUTS, given, strict=True))
    }
    for fetch in fetches.values():
        fetch.start()
    h, s = lax.axis_index("head"), lax.axis_index("seq")
    core = h % 2
    mate = h + 1 - 2 * core
    nxt, prv = (s + 1) % N_SEQ, (s + N_SEQ - 1) % N_SEQ
    weights = WeightGather(g, h, s)

    barrier = pltpu.get_barrier_semaphore()
    loop(1, N_HEAD, lambda d: greet(barrier, {"head": (h + d) % N_HEAD}))

    def greet_seq(d):
        greet(barrier, {"seq": (s + d) % N_SEQ})
        greet(barrier, {"seq": (s + d) % N_SEQ, "head": mate})

    loop(1, N_SEQ, greet_seq)

    @pl.when(h == 0)
    def _():
        loop(0, N_HEAD, lambda j: greet(barrier, {"seq": prv, "head": j}))

    def fetched(*names):
        for name in names:
            fetches[name].wait()

    fetched("x", "mix", "down")
    x = g.x[...].astype(F32)
    mix = g.mix[...]
    down_h, down_l = parts(g.down[...], 2)

    def into_rank(a):
        a_h, a_l = parts(a, 2)
        return mm(a_h, down_h) + (mm(a_h, down_l) + mm(a_l, down_h))

    g.part1[...] = into_rank(shift_mix(x, 0.0, mix)).reshape(N_HEAD, 8, 128)
    g.edge_part[...] = into_rank(mix * x[TOK - 8 :])
    g.land1[h] = g.part1[h]
    fetched("w")
    weights.keep_own()
    fetched("dy", "v", "r", "k", "u", "base", "up", "mixes")
    pl.semaphore_wait(barrier, N_HEAD - 1 + 2 * (N_SEQ - 1) + 1)
    in_first = AllToAll("head", N_HEAD, h, g.part1, g.land1, g.pair_sems, 0)
    in_first.start()
    edge_copy = remote(g.edge_part, g.edge_land.at[h], g.one.at[2], g.one.at[11], {"seq": nxt, "head": 0})
    edge_copy.start()
    weights.stage(0)
    row_copy = remote(g.x.at[pl.ds(TOK - 16, 16)], g.tail, g.one.at[0], g.one.at[1], {"seq": nxt})
    row_copy.start()

    rb, kb, vb, dyb = g.r[...], g.k[...], g.v[...], g.dy[...]
    r, k, v, dy = (a.astype(F32) for a in (rb, kb, vb, dyb))
    own = block_diagonal()
    odd = odd_rows()
    lane_head = head_of(iota((TOK, COL), 1))
    heads = [lane_head == i for i in range(4)]
    zero16 = jnp.zeros((TOK, COL), BF16)

    def by_head(a):
        return jnp.concatenate([jnp.where(m, a, zero16) for m in heads], axis=0)

    def lane_cat(stacked):
        return jnp.concatenate([stacked[i * TOK : (i + 1) * TOK] for i in range(4)], axis=1)

    spread = jnp.where(own, 1.0, 0.0).astype(BF16)
    unfold = jnp.where(iota((HS, COL), 0) == iota((HS, COL), 1) % HS, 1.0, 0.0).astype(BF16)
    head_rows = iota((8, COL), 0) == head_of(iota((8, COL), 1))
    u = jnp.concatenate([g.u[...], jnp.zeros((4, HS), F32)], axis=0)
    u = jnp.sum(jnp.where(head_rows, mm_right_exact(u, unfold, count=3), 0.0), axis=0, keepdims=True)

    def tiles(a):
        return a.reshape(TOK // 8, 8, COL)

    def flat(a):
        return a.reshape(TOK, COL)

    for i, piece in enumerate(parts(mm(by_head(dyb), vb, LANES_LANES), 2)):
        g.cross[i] = lane_cat(piece)
    for i, piece in enumerate(parts(mm(by_head(vb), dyb, LANES_LANES), 2)):
        g.cross[2 + i] = lane_cat(piece)
    for d in range(8):
        v_old = v if d == 0 else flat(pltpu.roll(tiles(v), d, 1))
        g.pairs[d] = mm_right_exact(dy * v_old, spread)

    in_first.wait_recv()

    @pl.when(h == 0)
    def _():
        remote(g.edge_land, g.edge_land, g.one.at[2], g.one.at[11], {"seq": nxt}).wait_recv()
        rows = g.edge_land[0]
        for j in range(1, N_HEAD):
            rows = rows + g.edge_land[j]
        first_row = jnp.where((iota((8, 128), 0) == 0) & (s > 0), pltpu.roll(rows, 1, 0), 0.0)
        g.land1[0] = g.land1[0] + first_row

    def summed(ref):
        acc = ref[0]
        for j in range(1, N_HEAD):
            acc = acc + ref[j]
        return acc

    g.full1[h] = summed(g.land1)
    in_second = AllToAll("head", N_HEAD, h, g.full1, g.full1, g.pair_sems, 1, True)
    in_second.start()
    weights.stage(1)
    in_second.wait_recv()

    mid = jnp.tanh(g.full1[...].reshape(TOK, RANK))
    up_h, up_l = parts(g.up[...], 2)
    mid_h, mid_l = parts(mid, 2)
    w = -jnp.exp(g.base[...] + (mm(mid_h, up_h) + (mm(mid_h, up_l) + mm(mid_l, up_h))))
    w_parts = parts(w, 3)
    ones = lower_ones(False)
    cumul = mm(ones, w_parts[0]) + (mm(ones, w_parts[1]) + mm(ones, w_parts[2]))
    before = cumul - w
    final = cumul[TOK - 1 : TOK]
    all_ones = jnp.ones((TOK, 128), BF16)
    w_turned = [p.astype(F32).T.astype(BF16) for p in w_parts]
    total_rows = mm(w_turned[0], all_ones) + (mm(w_turned[1], all_ones) + mm(w_turned[2], all_ones))
    to_end = jnp.exp(jnp.minimum(final - cumul, 0.0))
    from_start = jnp.exp(before)

    def folded(a, b):
        wide = jnp.where(own, mm_right_exact(a.T, b), 0.0)
        return wide[:, :128] + wide[:, 128:]

    state = folded(k * to_end, vb)
    grad = folded(r * from_start, dyb)
    packed = jnp.where(odd, pltpu.roll(state, 64, 1), state) + jnp.where(odd, grad, pltpu.roll(grad, 64, 1))
    g.pack[:, 0] = packed.reshape(N_SEQ, 8, 128)
    g.pack[:, 1] = jnp.exp(total_rows).reshape(N_SEQ, 8, 128)
    to_owner = AllToAll("seq", N_SEQ, s, g.pack, g.pack_in, g.pair_sems, 4)
    to_owner.start()
    g.pack_in[s] = g.pack[s]
    g.hold[0], g.hold[1], g.hold[2], g.hold[3] = w, cumul, to_end, from_start

    gr_mem = jnp.zeros((TOK, COL), F32)
    gk_in = jnp.zeros((TOK, COL), F32)
    score_st = jnp.zeros((4 * TOK, TOK), F32)
    tok = iota((TOK, COL), 0)

    def wide_mm(first, mask, factor):
        f_top, f_low = (by_head(p) for p in parts(factor, 2))
        zero = jnp.zeros((TOK, 4 * TOK), BF16)
        top, low = jnp.where(mask, g.cross[first], zero), jnp.where(mask, g.cross[first + 1], zero)
        return mm(top, f_top) + (mm(top, f_low) + mm(low, f_top))

    for half in (64, 32, 16, 8):
        size = 2 * half
        second = (tok % size) >= half
        middle = cumul.reshape(TOK // size, size, COL)[:, half - 1 : half]
        middle = jnp.broadcast_to(middle, (TOK // size, size, COL)).reshape(TOK, COL)
        fade = jnp.exp(jnp.minimum(jnp.where(second, before - middle, middle - cumul), 0.0))
        late, early = jnp.where(second, fade, 0.0), jnp.where(second, 0.0, fade)
        r_hat, k_hat = r * late, k * early
        same = iota((TOK, 4 * TOK), 0) // size == (iota((TOK, 4 * TOK), 1) % TOK) // size
        gr_mem = gr_mem + late * wide_mm(0, same, k_hat)
        gk_in = gk_in + early * wide_mm(2, same, r_hat)
        k_top, k_low = (by_head(p) for p in parts(k_hat, 2))
        r_top, r_low = parts(r_hat, 2)
        score = mm(k_top, r_top, LANES_LANES) + (mm(k_top, r_low, LANES_LANES) + mm(k_low, r_top, LANES_LANES))
        same_st = (iota((4 * TOK, TOK), 0) % TOK) // size == iota((4 * TOK, TOK), 1) // size
        score_st = score_st + jnp.where(same_st, score, 0.0)
    gv = jnp.zeros((TOK, COL), F32)
    dy_heads = by_head(dyb)
    for piece in parts(score_st, 2):
        gv = gv + mm(lane_cat(piece), dy_heads)

    weights.stage(2)
    to_owner.wait_recv()
    onward = jnp.zeros((8, 128), F32)
    forward = []
    for n in range(N_SEQ):
        forward.append(onward)
        onward = g.pack_in[n, 1] * onward + g.pack_in[n, 0]
    left8 = iota((8, 128), 1) < 64
    reverse = jnp.zeros((8, 128), F32)
    for n in reversed(range(N_SEQ)):
        g.back[n] = jnp.where(left8, forward[n], reverse)
        reverse = g.pack_in[n, 1] * reverse + g.pack_in[n, 0]
    to_range = AllToAll("seq", N_SEQ, s, g.back, g.got, g.pair_sems, 5)
    to_range.start()
    g.got[s] = g.back[s]

    sub = iota((TOK // 8, 8, COL), 1)
    for d in range(1, 8):
        valid = sub >= d
        cum_old = pltpu.roll(tiles(cumul), d, 1)
        k_old = flat(pltpu.roll(tiles(k), d, 1))
        fade = jnp.exp(jnp.minimum(jnp.where(valid, tiles(before) - cum_old, 0.0), 0.0))
        fade = flat(jnp.where(valid, fade, 0.0))
        pair = g.pairs[d]
        faded_r = fade * r
        gr_mem = gr_mem + fade * pair * k_old
        gk_in = gk_in + flat(pltpu.roll(tiles(faded_r * pair), 8 - d, 1))
        score = mm_right_exact(faded_r * k_old, spread)
        gv = gv + flat(pltpu.roll(tiles(score * dy), 8 - d, 1))
    gv = gv + mm_right_exact(r * u * k, spread) * dy
    g.hold[4], g.hold[5], g.hold[6] = gr_mem, gk_in, gv
    weights.stage(3)
    to_range.wait_recv()

    w, cumul, to_end, from_start = g.hold[0], g.hold[1], g.hold[2], g.hold[3]
    packed = g.got[...].reshape(COL, 128)
    left = iota((COL, 128), 1) < 64
    state, grad = jnp.where(left, packed, 0.0), jnp.where(left, 0.0, packed)
    state = jnp.where(odd, pltpu.roll(state, 64, 1), state)
    grad = jnp.where(odd, grad, pltpu.roll(grad, 64, 1))
    state = jnp.where(own, jnp.concatenate([state, state], axis=1), 0.0)
    grad = jnp.where(own, jnp.concatenate([grad, grad], axis=1), 0.0)
    gr_mem = g.hold[4] + from_start * mm_left_exact(dyb, state, LANES_LANES)
    gk_in = g.hold[5]
    gk_out = to_end * mm_left_exact(vb, grad, LANES_LANES)
    across = mm_left_exact(jnp.ones((8, COL), BF16), state * grad, LANES_LANES, 3)[0:1]
    across = across * jnp.exp(cumul[TOK - 1 : TOK])
    k_in = k * gk_in
    g_log = across - k_in + mm_left_exact(lower_ones(True), k * gk_out)
    g_log = g_log + mm_left_exact(upper_ones(), r * gr_mem - k_in)
    g_pre = g_log * w
    g.part2[...] = mm3(g_pre, g.up[...], LANES_LANES).reshape(N_HEAD, 8, 128)
    out_first = AllToAll("head", N_HEAD, h, g.part2, g.land2, g.pair_sems, 2)
    out_first.start()
    g.land2[h] = g.part2[h]

    self_pair = g.pairs[0]
    r_pair = r * self_pair
    g.proj[core, 0] = (gr_mem + u * k * self_pair).astype(BF16)
    g.proj[core, 1] = (gk_in + gk_out + u * r_pair).astype(BF16)
    g.proj[core, 2] = (g.hold[6] + mm3(k * to_end, grad)).astype(BF16)
    swap = remote(g.proj.at[core], g.proj.at[core], g.one.at[3], g.one.at[4], {"head": mate})
    first_rows = g.proj.at[core, :, pl.ds(0, 16)]
    near = remote(first_rows, g.proj_edge.at[core], g.one.at[5], g.one.at[6], {"seq": prv})
    far = remote(first_rows, g.proj_edge.at[core], g.one.at[7], g.one.at[8], {"seq": prv, "head": mate})
    swap.start()
    near.start()
    far.start()
    raising = mm3(mid.T, g_pre)
    g.rise[0:16, 0:8] = raising[:, 0:128].reshape(16, 8, 128)
    g.rise[16:32, 0:8] = raising[:, 128:256].reshape(16, 8, 128)
    floor_row = jnp.sum(g_pre, axis=0, keepdims=True)
    bonus_row = jnp.sum(k * r_pair, axis=0, keepdims=True)
    row8 = iota((8, 128), 0)
    small = jnp.where(row8 == 0, floor_row[:, :128], 0.0) + jnp.where(row8 == 1, floor_row[:, 128:], 0.0)
    small = small + jnp.where(row8 == 2, bonus_row[:, :128], 0.0) + jnp.where(row8 == 3, bonus_row[:, 128:], 0.0)
    g.rise[:, 8:16] = jnp.broadcast_to(small[None], (N_SEQ, 8, 128))
    rise_first = AllToAll("seq", N_SEQ, s, g.rise, g.rise_in, g.pair_sems, 6)
    rise_first.start()
    g.rise_in[s] = g.rise[s]
    row_copy.wait()
    carried = jnp.where(s == 0, 0.0, g.tail[...].astype(F32)[15:16])
    turned_in = shift_mix(x, carried, mix).T

    out_first.wait_recv()
    g.full2[h] = summed(g.land2)
    out_second = AllToAll("head", N_HEAD, h, g.full2, g.full2, g.pair_sems, 3, True)
    out_second.start()
    weights.stage(4)

    swap.wait()
    near.wait()
    far.wait()
    for c in range(2):
        for m in range(3):
            a = g.proj[c, m].astype(F32)
            edge = jnp.where(s == N_SEQ - 1, 0.0, g.proj_edge[c, m].astype(F32)[0:1])
            later = jnp.where(tok == TOK - 1, edge, pltpu.roll(a, TOK - 1, 0))
            g.turned[c, m, :, 0:TOK] = a.T.astype(BF16)
            g.turned[c, m, :, TOK:] = later.T.astype(BF16)
    for pair in range(4):
        columns = []
        for i in range(4):
            for p in range(2):
                place = 8 * i + 2 * pair + p
                column = g.mixes[:, place * 128 : (place + 1) * 128].T
                columns.append(jnp.where(core == 0, column[:64], column[64:]))
        g.mix_columns[pair] = jnp.concatenate(columns, axis=0)
    out_second.wait_recv()

    g_mid = g.full2[...].reshape(TOK, RANK) * (1.0 - mid * mid)
    g.fall[...] = mm3(turned_in, g_mid).reshape(N_SEQ, 8, 128)
    fall_first = AllToAll("seq", N_SEQ, s, g.fall, g.fall_in, g.pair_sems, 7)
    fall_first.start()
    gdi = mm3(g_mid, g.down[...], LANES_LANES)
    g.gdi[...] = gdi
    edge_row = remote(g.gdi.at[pl.ds(0, 8)], g.gdi_edge, g.one.at[9], g.one.at[10], {"seq": prv})
    edge_row.start()
    g.fall_in[s] = g.fall[s]

    def summed_seq(ref):
        acc = ref[0]
        for n in range(1, N_SEQ):
            acc = acc + ref[n]
        return acc

    y_copy = AllToAll("head", N_HEAD, h, g.y_out, g.y_in, g.pair_sems, 10)
    near_pair = (s % 8) // 2
    for turn in (0, 1, 3, 2):
        pair = (near_pair + turn) % 4
        if turn == 1:
            weights.stage(5)
        if turn == 2:
            fall_first.wait_recv()
            g.fall_total[s] = summed_seq(g.fall_in)
            fall_second = AllToAll("seq", N_SEQ, s, g.fall_total, g.fall_total, g.pair_sems, 9, True)
            fall_second.start()
            weights.stage(6)
        weights.far_side(2 * pair)
        weights.far_side(2 * pair + 1)
        mixes = g.mix_columns[pair]
        acc = jnp.zeros((4 * TOK, TOK), F32)
        for m in range(3):
            term = None
            for c in range(2):
                rows = g.buf[:, pl.ds(2 * pair, 2), c, m].reshape(4 * TOK, COL)
                one = mm(rows, g.turned[c, m])
                term = one if term is None else term + one
            here, there = term[:, :TOK], term[:, TOK:]
            acc = acc + here + mixes[:, m : m + 1] * (there - here)
        for i in range(4):
            to = 4 * i + pair
            g.y_out[to] = acc[i * TOK : (i + 1) * TOK].astype(BF16)

            @pl.when(to != h)
            def _():
                y_copy.start_one(to)

        if turn == 0:
            rise_first.wait_recv()
            acc = summed_seq(g.rise_in)
            g.rise_total[s] = acc[:8]
            rise_second = AllToAll("seq", N_SEQ, s, g.rise_total, g.rise_total, g.pair_sems, 8, True)
            rise_second.start()
            g.base_grad[:, 0:128] = acc[8:9]
            g.base_grad[:, 128:256] = acc[9:10]
            bonus = jnp.concatenate([acc[10:11], acc[11:12]], axis=1)
            bonus = jnp.where(head_rows, bonus, 0.0)
            rows = None
            for piece in parts(bonus, 3):
                one = mm(piece, unfold, LANES_LANES)
                rows = one if rows is None else rows + one
            g.bonus_grad[...] = rows

    edge_row.wait()
    gdi = g.gdi[...]
    next_row = jnp.where(s == N_SEQ - 1, 0.0, g.gdi_edge[0:1])
    later = jnp.where(tok == TOK - 1, next_row, pltpu.roll(gdi, TOK - 1, 0))
    mine = gdi + mix * (later - gdi)
    g.y_in[h] = g.y_out[h]
    y_copy.wait_recv()
    halves = []
    for c in range(2):
        acc = g.y_in[c].astype(F32)
        for y in range(1, 8):
            acc = acc + g.y_in[2 * y + c].astype(F32)
        halves.append(acc)
    lo, hi = halves
    joined = jnp.concatenate([lo[:64], hi[:64], lo[64:], hi[64:]], axis=0)
    g.out[...] = (joined.T + mine).astype(BF16)

    edge_copy.wait_send()
    for copies in (
        in_first, in_second, out_first, out_second, to_owner, to_range, rise_first, rise_second, fall_first, y_copy,
    ):
        copies.wait_send()
    weights.wait_send()
    rise_second.wait_recv()
    g.up_grad[:, 0:128] = g.rise_total[0:16].reshape(RANK, 128)
    g.up_grad[:, 128:256] = g.rise_total[16:32].reshape(RANK, 128)
    fall_second.wait_recv()
    g.down_grad[...] = g.fall_total[...].reshape(COL, RANK)
    fall_second.wait_send()


def step(*operands):
    return pl.pallas_call(
        step_kernel,
        out_shape=tuple(jax.ShapeDtypeStruct(*spec) for spec in OUTPUTS.values()),
        in_specs=[pl.BlockSpec(memory_space=pl.ANY)] * len(INPUTS),
        out_specs=(VMEM,) * len(OUTPUTS),
        scratch_shapes=list(SCRATCH.values()),
        compiler_params=pltpu.CompilerParams(
            collective_id=0, has_side_effects=True, vmem_limit_bytes=60 * 2**20
        ),
        name="step",
    )(*operands)


def finish_kernel(out_in, down_in, up_in, base_in, bonus_in, out, down_grad, up_grad, base_grad, bonus_grad):
    out[...] = out_in[...]
    down_grad[...] = down_in[...]
    up_grad[...] = up_in[...]
    base_grad[...] = base_in[...].reshape(COL)
    bonus_grad[...] = bonus_in[0:4]


def finish(*results):
    return pl.pallas_call(
        finish_kernel,
        out_shape=(
            *(jax.ShapeDtypeStruct(*spec) for spec in list(OUTPUTS.values())[:3]),
            jax.ShapeDtypeStruct((COL,), F32),
            jax.ShapeDtypeStruct((4, HS), F32),
        ),
        in_specs=[VMEM] * 5,
        out_specs=(VMEM,) * 5,
        name="finish",
    )(*results)


def per_device(
    layer_input, receptance, key_act, value_act, attention_result_sensitivity, time_first,
    decay_exponent_base, decay_shift_mix, mix_rkv, decay_adapter_down, decay_adapter_up, proj_weights,
):
    given = {
        "x": layer_input, "mix": decay_shift_mix[None], "down": decay_adapter_down,
        "base": decay_exponent_base[None], "up": decay_adapter_up, "r": receptance, "k": key_act,
        "v": value_act, "dy": attention_result_sensitivity, "u": time_first, "w": proj_weights, "mixes": mix_rkv,
    }
    return finish(*step(*(given[name] for name in INPUTS)))


def solution(mesh):
    return jax.shard_map(
        per_device,
        mesh=mesh,
        in_specs=(
            P("seq", "head"), P("seq", "head"), P("seq", "head"), P("seq", "head"), P("seq", "head"),
            P("head", None), P("head"), P("head"), P(), P("head", None), P(None, "head"),
            P(None, "seq", "head"),
        ),
        out_specs=(P("seq", "head"), P("head", None), P(None, "head"), P("head"), P("head", None)),
        check_vma=False,
    )
```
